32 devices in a mesh: ctx: 16 (over z, x, core), head: 2 (over y).
Axes of the slice: x: 2, y: 2, z: 4, core: 2. Of those that a mesh axis runs over, the one named last changes fastest.
Arguments:
- queries: bfloat16 [4096, 1024], P('ctx', 'head'), may hold values from -6 to 6
- keys: bfloat16 [4096, 1024], P('ctx', 'head'), may hold values from -6 to 6
- values: bfloat16 [4096, 1024], P('ctx', 'head'), may hold values from -6 to 6
- out_grad: bfloat16 [4096, 1024], P('ctx', 'head'), may hold values from -48 to 48
- outputs: bfloat16 [4096, 1024], P('ctx', 'head'), may hold values from -1.5 to 1.5
- log_norms: float32 [4096, 8], P('ctx', 'head'), may hold values from 4 to 7
- selected: int32 [32, 8, 3], P('ctx', 'head'), may hold values from -1 to 29, as said below
Outputs:
- grad_queries: bfloat16 [4096, 1024], P(('ctx', 'head'))
- grad_keys: bfloat16 [4096, 1024], P('ctx', 'head')
- grad_values: bfloat16 [4096, 1024], P('ctx', 'head')
The draws below stay inside these ranges and needn't reach their ends.
Inputs may be any that keep to these rules, and one draw needn't show every extreme that they name: `selected`: -1 marks no block; every other entry is a block held by a lower index of ctx than the query block's own, and the entries other than -1 of one query block and head differ. Among all entries of one index of ctx and one group of 4 heads, at most 2 name blocks held by any one other index of ctx; blocks may repeat across query blocks and heads.
All inputs are finite; a program needn't handle non-finite values.
Results may differ from the reference program's by a relative error of at most 0.0057.
Values may be sent and summed in bfloat16 or wider, within the bound.
A program may use at most 64 MiB of HBM per device.

```python
import jax
import jax.numpy as jnp
from jax import lax

DH = 128
HEADS_DEV = 4
TOPK = 3
PER_PEER = 2
BLK_DEV = 2
HEADS = 8
BLOCK_COUNT = 32
TOKENS = 4096
N_CTX = 16
N_HEAD = 2


def choose_blocks(seed_key, device_position, block_demand, busiest_device):
    slot_count = BLK_DEV * HEADS_DEV * TOPK
    block_numbers = jnp.arange(BLOCK_COUNT, dtype=jnp.int32)
    owning_devices = block_numbers // BLK_DEV
    device_ids = jnp.arange(N_CTX, dtype=jnp.int32)
    random_jitter = jax.random.randint(seed_key, (slot_count, BLOCK_COUNT), 0, 1 << 15, dtype=jnp.int32)
    extra_reward = jnp.where(owning_devices == busiest_device, 1 << 19, 0).astype(jnp.int32)
    block_scores = (random_jitter * block_demand[None, :] + extra_reward[None, :]) * BLOCK_COUNT + block_numbers[None, :]
    earlier = block_numbers < device_position * BLK_DEV

    def step(carry, inputs):
        counts, taken = carry
        row, index = inputs
        taken = jnp.where(index % TOPK == 0, jnp.zeros_like(taken), taken)
        valid = earlier & (taken == 0) & (counts[owning_devices] < PER_PEER)
        masked = jnp.where(valid, row, -1)
        best = jnp.argmax(masked).astype(jnp.int32)
        found = jnp.any(valid)
        choice_made = jnp.where(found, best, -1).astype(jnp.int32)
        counts = counts + jnp.where(found & (device_ids == best // BLK_DEV), 1, 0).astype(jnp.int32)
        taken = taken + jnp.where(found & (block_numbers == best), 1, 0).astype(jnp.int32)
        return ((counts, taken), choice_made)
    start = (jnp.zeros((N_CTX,), jnp.int32), jnp.zeros((BLOCK_COUNT,), jnp.int32))
    ignored, picks = lax.scan(step, start, (block_scores, jnp.arange(slot_count, dtype=jnp.int32)))
    return picks


def draw_selected(key, part):
    popular_key, base_key = jax.random.split(jax.random.fold_in(key, 17), 2)
    block_demand = jax.random.randint(popular_key, (BLOCK_COUNT,), 1, 9, dtype=jnp.int32)
    busiest_device = jnp.zeros((), jnp.int32)

    def single_draw(position):
        return choose_blocks(jax.random.fold_in(base_key, position), position // N_HEAD, block_demand, busiest_device)
    flat = jax.vmap(single_draw)(jnp.arange(N_CTX * N_HEAD, dtype=jnp.int32))
    grid = flat.reshape(N_CTX, N_HEAD, BLK_DEV, HEADS_DEV, TOPK)
    grid = jnp.transpose(grid, (0, 2, 1, 3, 4))
    return grid.reshape(BLOCK_COUNT, HEADS, TOPK)


def block_scale(key, shape, shards, low, top_value):
    level = 1.0
    for axis_at, shards_of in shards:
        heights = jax.random.uniform(jax.random.fold_in(jax.random.fold_in(key, 6), axis_at), (shards_of,), jnp.float32, low / len(shards), top_value / len(shards))
        level = level * jnp.repeat(jnp.exp(heights), shape[axis_at] // shards_of).reshape((-1,) + (1,) * (len(shape) - 1 - axis_at))
    return level


def gaussian(rng, extent, spread, reach, shards=(), kind=jnp.bfloat16):
    array = spread * jax.random.normal(rng, extent, jnp.float32)
    if shards:
        array = array * block_scale(rng, extent, shards, -0.22, 0.18)
    return jnp.clip(array, -reach, reach).astype(kind)


def setup_inputs(seed: int = 0) -> dict:
    key_of = jax.random.split(jax.random.key(seed), 8)
    queries = gaussian(key_of[0], (TOKENS, HEADS * DH), 1.0, 6.0, ((0, 16), (1, 2)))
    keys = gaussian(key_of[1], (TOKENS, HEADS * DH), 1.0, 6.0, ((0, 16), (1, 2)))
    values = gaussian(key_of[2], (TOKENS, HEADS * DH), 1.0, 6.0, ((0, 16), (1, 2)))
    out_grad = gaussian(key_of[3], (TOKENS, HEADS * DH), 8.0, 48.0, ((0, 16), (1, 2)))
    outputs = gaussian(key_of[4], (TOKENS, HEADS * DH), 0.25, 1.5, ((0, 16), (1, 2)))
    log_norms = jnp.clip(4.0 + 3.0 * jax.random.uniform(key_of[5], (TOKENS, HEADS), jnp.float32) ** block_scale(key_of[5], (TOKENS, HEADS), ((0, 16), (1, 2)), -0.2, 0.2), 4.0, 7.0)
    selected = draw_selected(jax.random.fold_in(key_of[7], 71), 0)
    return dict(queries=queries, keys=keys, values=values, out_grad=out_grad, outputs=outputs, log_norms=log_norms, selected=selected)


def settle(terms):
    own = terms[:, :1]
    rest = lax.optimization_barrier(terms[:, 1:].astype(jnp.bfloat16)).astype(jnp.float32)
    return jnp.concatenate([own, rest], axis=1)


def head_grads(queries, keys, values, out_grad, outputs, log_norms, selected, column):
    tokens = queries.shape[0]
    heads = log_norms.shape[1]
    head_dim = queries.shape[1] // heads
    blocks = selected.shape[0]
    top_count = selected.shape[2]
    block_len = tokens // blocks
    factor = head_dim ** -0.5
    start = column * head_dim

    def pick(matrix):
        piece = lax.dynamic_slice_in_dim(matrix, start, head_dim, 1)
        return piece.astype(jnp.float32).reshape(blocks, block_len, head_dim)

    query_rows = pick(queries)
    key_rows = pick(keys)
    value_rows = pick(values)
    grad_rows = pick(out_grad)
    output_rows = pick(outputs)
    norms = lax.dynamic_index_in_dim(log_norms, column, 1, keepdims=False).reshape(blocks, block_len)
    deltas = jnp.sum(grad_rows * output_rows, axis=2)
    chosen = lax.dynamic_index_in_dim(selected, column, 1, keepdims=False)
    listed = jnp.concatenate([jnp.arange(blocks, dtype=jnp.int32)[:, None], chosen.astype(jnp.int32)], axis=1)
    alive = listed >= 0
    safe = jnp.where(alive, listed, 0).astype(jnp.int32)
    slots = top_count + 1
    key_width = slots * block_len
    key_sel = key_rows[safe].reshape(blocks, key_width, head_dim)
    value_sel = value_rows[safe].reshape(blocks, key_width, head_dim)
    position = jnp.arange(block_len)
    lower = position[:, None] >= position[None, :]
    slot_rule = jnp.concatenate([lower[None], jnp.ones((top_count, block_len, block_len), dtype=bool)], axis=0)
    allowed = slot_rule[None] & alive[:, :, None, None]
    allowed = jnp.transpose(allowed, (0, 2, 1, 3)).reshape(blocks, block_len, key_width)
    block_scores = jnp.einsum("nsd,nkd->nsk", query_rows, key_sel) * factor
    weights = jnp.where(allowed, jnp.exp(block_scores - norms[:, :, None]), 0.0)
    dweights = jnp.einsum("nsd,nkd->nsk", grad_rows, value_sel)
    dscores = weights * (dweights - deltas[:, :, None])
    weights_b = lax.optimization_barrier(weights.astype(jnp.bfloat16)).astype(jnp.float32)
    dscores_b = lax.optimization_barrier(dscores.astype(jnp.bfloat16)).astype(jnp.float32)
    dscore_four = dscores_b.reshape(blocks, block_len, slots, block_len)
    weight_four = weights_b.reshape(blocks, block_len, slots, block_len)
    key_four = key_sel.reshape(blocks, slots, block_len, head_dim)
    query_terms = jnp.einsum("nsjk,njkd->njsd", dscore_four, key_four) * factor
    key_terms = jnp.einsum("nsjk,nsd->njkd", dscore_four, query_rows) * factor
    value_terms = jnp.einsum("nsjk,nsd->njkd", weight_four, grad_rows)
    live_weight = alive.astype(jnp.float32)[:, :, None, None]
    grad_q = jnp.sum(settle(query_terms) * live_weight, axis=1)
    part_k = settle(key_terms) * live_weight
    part_v = settle(value_terms) * live_weight
    flat_index = safe.reshape(-1)
    grad_k = jnp.zeros((blocks, block_len, head_dim), jnp.float32).at[flat_index].add(part_k.reshape(-1, block_len, head_dim))
    grad_v = jnp.zeros((blocks, block_len, head_dim), jnp.float32).at[flat_index].add(part_v.reshape(-1, block_len, head_dim))
    return grad_q, grad_k, grad_v


def reference(queries, keys, values, out_grad, outputs, log_norms, selected):
    tokens, full_width = queries.shape
    heads = log_norms.shape[1]
    head_dim = full_width // heads

    def per_head(column):
        return head_grads(queries, keys, values, out_grad, outputs, log_norms, selected, column)

    grad_q, grad_k, grad_v = lax.map(per_head, jnp.arange(heads, dtype=jnp.int32))

    def merge_heads(stack):
        stack = stack.reshape(heads, tokens, head_dim)
        return jnp.transpose(stack, (1, 0, 2)).reshape(tokens, full_width).astype(jnp.bfloat16)

    return merge_heads(grad_q), merge_heads(grad_k), merge_heads(grad_v)
```

```python
import functools

import jax
import jax.numpy as jnp
from jax import lax
from jax.experimental import pallas as pl
from jax.experimental.pallas import tpu as pltpu
from jax.sharding import PartitionSpec as P

GROUP = 4
JOBS_STEP = 4
MESH_ID = pl.DeviceIdType.MESH
NT = (((1,), (1,)), ((), ()))
NN = (((1,), (0,)), ((), ()))


def gather_kernel(levels, q_ref, g_ref, k_ref, v_ref, m_ref, a_buf, b_buf, m_buf, send_sem, recv_sem):
    me = lax.axis_index("ctx")
    head = lax.axis_index("head")
    level = me // GROUP
    col = me % GROUP
    colx = (col + 2) % GROUP
    colc = col + 1 - 2 * (col % 2)
    down_dev = me - GROUP
    up_dev = me + GROUP
    x_dev = level * GROUP + colx
    c_dev = level * GROUP + colc
    bufs = (a_buf, b_buf, m_buf)
    down_own = (q_ref, g_ref, m_ref)
    up_own = (k_ref, v_ref, m_ref)
    has_down = level > 0
    has_up = level < levels - 1

    barrier = pltpu.get_barrier_semaphore()

    def greet(dev):
        pl.semaphore_signal(barrier, inc=1, device_id=(dev, head), device_id_type=MESH_ID)

    greet(x_dev)
    greet(c_dev)

    @pl.when(has_down)
    def _():
        greet(down_dev)

    @pl.when(has_up)
    def _():
        greet(up_dev)

    pl.semaphore_wait(barrier, 2 + has_down.astype(jnp.int32) + has_up.astype(jnp.int32))

    def copy(way, part, slot, src, dev):
        return pltpu.make_async_remote_copy(
            src_ref=src,
            dst_ref=bufs[part].at[slot],
            send_sem=send_sem.at[way, part, slot],
            recv_sem=recv_sem.at[part, slot],
            device_id=(dev, head),
            device_id_type=MESH_ID,
        )

    def push(way, slot, dev, own=None):
        for part in (2, 0, 1):
            src = bufs[part].at[slot] if own is None else own[part]
            copy(way, part, slot, src, dev).start()

    def push_part(way, part, slot, dev):
        copy(way, part, slot, bufs[part].at[slot], dev).start()

    def arrive(part, slot):
        copy(0, part, slot, bufs[part].at[slot], c_dev).wait_recv()

    def sent(way, slot):
        for part in range(3):
            copy(way, part, slot, bufs[part].at[slot], c_dev).wait_send()

    @pl.when(has_down)
    def _():
        push(0, me, down_dev, down_own)

    @pl.when(has_up)
    def _():
        push(3, me, up_dev, up_own)

    @pl.when(col >= 2)
    def _():
        push(1, me, x_dev, down_own)

    @pl.when(col < 2)
    def _():
        push(1, me, x_dev, up_own)

    @pl.when(col % 2 == 1)
    def _():
        push(2, me, c_dev, down_own)

    @pl.when(col % 2 == 0)
    def _():
        push(2, me, c_dev, up_own)

    def cross(other):
        slot = other * GROUP + colx
        for part in (2, 0, 1):
            arrive(part, slot)
            push_part(2, part, slot, c_dev)

    def step(dist, carry):
        high = level + dist
        low = level - dist

        @pl.when(high < levels)
        def _():
            slot = high * GROUP + col
            for part in (2, 0, 1):
                arrive(part, slot)

                @pl.when(has_down)
                def _():
                    push_part(0, part, slot, down_dev)

                push_part(1, part, slot, x_dev)
                push_part(2, part, slot, c_dev)

        @pl.when(low >= 0)
        def _():
            slot = low * GROUP + col
            for part in (2, 0, 1):
                arrive(part, slot)

                @pl.when(has_up)
                def _():
                    push_part(0, part, slot, up_dev)

                push_part(1, part, slot, x_dev)
                push_part(2, part, slot, c_dev)

        before = dist - 1

        @pl.when(level + before < levels)
        def _():
            cross(level + before)

        @pl.when((before > 0) & (level - before >= 0))
        def _():
            cross(level - before)

        return carry

    lax.fori_loop(1, levels + 1, step, 0)

    def finish(other, carry):
        for column in (colc, (colc + 2) % GROUP):
            for part in range(3):
                arrive(part, other * GROUP + column)
        own_slot = other * GROUP + col
        sent(1, own_slot)
        sent(2, own_slot)
        sent(2, other * GROUP + colx)

        @pl.when(has_down & (other >= level))
        def _():
            sent(0, own_slot)

        @pl.when(has_up & (other < level))
        def _():
            sent(0, own_slot)

        @pl.when(has_up & (other == level))
        def _():
            sent(3, own_slot)

        return carry

    lax.fori_loop(0, levels, finish, 0)


def gather(queries, out_grad, keys, values, meta):
    count = lax.axis_size("ctx")
    rows = queries.shape
    anywhere = pl.BlockSpec(memory_space=pl.ANY)
    return pl.pallas_call(
        functools.partial(gather_kernel, count // GROUP),
        out_shape=(
            jax.ShapeDtypeStruct((count,) + rows, queries.dtype),
            jax.ShapeDtypeStruct((count,) + rows, queries.dtype),
            jax.ShapeDtypeStruct((count,) + meta.shape, meta.dtype),
        ),
        in_specs=[anywhere] * 5,
        out_specs=(anywhere,) * 3,
        scratch_shapes=[
            pltpu.SemaphoreType.DMA((4, 3, count)),
            pltpu.SemaphoreType.DMA((3, count)),
        ],
        compiler_params=pltpu.CompilerParams(collective_id=0, has_side_effects=True),
    )(queries, out_grad, keys, values, meta)


def dot(left, right, dims):
    return lax.dot_general(left, right, dims, preferred_element_type=jnp.float32)


def compute_kernel(
    blocks, heads, top, block_len, dh, factor,
    tab_ref, sel_ref,
    q_ref, g_ref, k_ref, v_ref, stat_ref, own_ref, m_buf, a_buf, b_buf,
    dq_ref, dk_ref, dv_ref,
    jq, jg, sk, sv, kacc, vacc, job_src, job_pair, job_key, job_sem, sel_sem,
):
    me = lax.axis_index("ctx")
    count = m_buf.shape[0]
    pairs = blocks * heads
    per_dev = pairs * top
    first = me * blocks

    def where_of(ref, dev, block, head):
        return ref.at[dev, pl.ds(block * block_len, block_len), pl.ds(head * dh, dh)]

    def own_of(ref, block, head):
        return ref.at[pl.ds(block * block_len, block_len), pl.ds(head * dh, dh)]

    for entry in range(per_dev):
        chosen = sel_ref[entry]
        block, head = entry // top // heads, entry // top % heads

        @pl.when(chosen >= 0)
        def _():
            dev, inner = chosen // blocks, chosen % blocks
            pltpu.make_async_copy(where_of(a_buf, dev, inner, head), sk.at[entry], sel_sem.at[0, entry]).start()
            pltpu.make_async_copy(where_of(b_buf, dev, inner, head), sv.at[entry], sel_sem.at[1, entry]).start()

        @pl.when(chosen < 0)
        def _():
            pltpu.make_async_copy(own_of(k_ref, block, head), sk.at[entry], sel_sem.at[0, entry]).start()
            pltpu.make_async_copy(own_of(v_ref, block, head), sv.at[entry], sel_sem.at[1, entry]).start()

    def scan(dev, found):
        for entry in range(per_dev):
            chosen = tab_ref[dev * per_dev + entry]
            block, head = entry // top // heads, entry // top % heads
            hit = (chosen >= first) & (chosen < first + blocks)

            @pl.when(hit)
            def _():
                job_src[found] = dev
                job_pair[found] = entry // top
                job_key[found] = (chosen - first) * heads + head
                pltpu.make_async_copy(where_of(a_buf, dev, block, head), jq.at[found], job_sem.at[0, found]).start()
                pltpu.make_async_copy(where_of(b_buf, dev, block, head), jg.at[found], job_sem.at[1, found]).start()

            found = found + hit.astype(jnp.int32)
        return found

    found = lax.fori_loop(me + 1, count, scan, jnp.int32(0))

    def owner_terms(keys, vals, qs, gs, norm, delta, causal):
        scores = dot(keys, qs, NT) * factor
        weights = jnp.exp(scores - norm)
        if causal:
            at_key = lax.broadcasted_iota(jnp.int32, scores.shape, 0)
            at_query = lax.broadcasted_iota(jnp.int32, scores.shape, 1)
            weights = jnp.where(at_key <= at_query, weights, 0.0)
        dweights = dot(vals, gs, NT)
        dscores = (weights * (dweights - delta)).astype(jnp.bfloat16)
        return dot(dscores, qs, NN) * factor, dot(weights.astype(jnp.bfloat16), gs, NN)

    def piece(ref, block, head):
        return ref[block * block_len:(block + 1) * block_len, head * dh:(head + 1) * dh]

    for pair in range(pairs):
        block, head = pair // heads, pair % heads
        part_k, part_v = owner_terms(
            piece(k_ref, block, head), piece(v_ref, block, head),
            piece(q_ref, block, head), piece(g_ref, block, head),
            own_ref[pair:pair + 1, :], own_ref[pairs + pair:pairs + pair + 1, :], True,
        )
        kacc[pair] = part_k
        vacc[pair] = part_v

    for entry in range(per_dev):
        pltpu.make_async_copy(own_of(k_ref, 0, 0), sk.at[entry], sel_sem.at[0, entry]).wait()
        pltpu.make_async_copy(own_of(v_ref, 0, 0), sv.at[entry], sel_sem.at[1, entry]).wait()
    wide = top * block_len
    for pair in range(pairs):
        block, head = pair // heads, pair % heads
        qs, gs = piece(q_ref, block, head), piece(g_ref, block, head)
        own_k, own_v = piece(k_ref, block, head), piece(v_ref, block, head)
        rows = slice(block * block_len, (block + 1) * block_len)
        norm = stat_ref[rows, head:head + 1]
        delta = stat_ref[rows, heads + head:heads + head + 1]
        far_k = sk[pair * top:(pair + 1) * top].reshape(wide, dh)
        far_v = sv[pair * top:(pair + 1) * top].reshape(wide, dh)
        weights = jnp.exp(dot(qs, own_k, NT) * factor - norm)
        at_query = lax.broadcasted_iota(jnp.int32, weights.shape, 0)
        at_key = lax.broadcasted_iota(jnp.int32, weights.shape, 1)
        weights = jnp.where(at_key <= at_query, weights, 0.0)
        near = (weights * (dot(gs, own_v, NT) - delta)).astype(jnp.bfloat16)
        weights = jnp.exp(dot(qs, far_k, NT) * factor - norm)
        far = weights * (dot(gs, far_v, NT) - delta)
        parts = []
        for turn in range(top):
            part = far[:, turn * block_len:(turn + 1) * block_len]
            parts.append(jnp.where(sel_ref[pair * top + turn] >= 0, part, 0.0))
        far = jnp.concatenate(parts, axis=1).astype(jnp.bfloat16)
        total = (dot(near, own_k, NN) + dot(far, far_k, NN)) * factor
        dq_ref[rows, head * dh:(head + 1) * dh] = total.astype(dq_ref.dtype)

    def drain(job, carry):
        pltpu.make_async_copy(own_of(k_ref, 0, 0), jq.at[job], job_sem.at[0, job]).wait()
        pltpu.make_async_copy(own_of(v_ref, 0, 0), jg.at[job], job_sem.at[1, job]).wait()
        return carry

    lax.fori_loop(0, found, drain, 0)

    def turn(step, carry):
        results = []
        for lane in range(JOBS_STEP):
            job = step * JOBS_STEP + lane
            live = job < found
            job = jnp.minimum(job, found - 1)
            key = job_key[job]
            src, pair = job_src[job], job_pair[job]
            block, head = key // heads, key % heads
            rows = pl.ds(pl.multiple_of(block * block_len, block_len), block_len)
            cols = pl.ds(pl.multiple_of(head * dh, dh), dh)
            part_k, part_v = owner_terms(
                k_ref[rows, cols], v_ref[rows, cols], jq[job], jg[job],
                m_buf[src, pl.ds(pair, 1), :], m_buf[src, pl.ds(pairs + pair, 1), :], False,
            )
            results.append((key, jnp.where(live, part_k, 0.0), jnp.where(live, part_v, 0.0)))
        for key, part_k, part_v in results:
            kacc[key] += part_k
            vacc[key] += part_v
        return carry

    lax.fori_loop(0, (found + JOBS_STEP - 1) // JOBS_STEP, turn, 0)
    for pair in range(pairs):
        block, head = pair // heads, pair % heads
        rows = slice(block * block_len, (block + 1) * block_len)
        dk_ref[rows, head * dh:(head + 1) * dh] = kacc[pair].astype(dk_ref.dtype)
        dv_ref[rows, head * dh:(head + 1) * dh] = vacc[pair].astype(dv_ref.dtype)


def stat_pairs(matrix, blocks):
    row_count, heads = matrix.shape
    shaped = matrix.reshape(blocks, row_count // blocks, heads)
    return jnp.transpose(shaped, (0, 2, 1)).reshape(blocks * heads, row_count // blocks)


def shards(queries, keys, values, out_grad, outputs, log_norms, selected):
    blocks, heads, top = selected.shape
    row_count, width = queries.shape
    dh = width // heads
    block_len = row_count // blocks
    pairs = blocks * heads
    count = lax.axis_size("ctx")
    per_dev = pairs * top
    deltas = jnp.sum(
        (out_grad.astype(jnp.float32) * outputs.astype(jnp.float32)).reshape(row_count, heads, dh), axis=2
    )
    stats = jnp.concatenate([log_norms, deltas], axis=1)
    chosen = selected.reshape(pairs, top).astype(jnp.float32)
    chosen = jnp.pad(chosen, ((0, 0), (0, block_len - top)))
    meta = jnp.concatenate([stat_pairs(log_norms, blocks), stat_pairs(deltas, blocks), chosen], axis=0)
    a_buf, b_buf, m_buf = gather(queries, out_grad, keys, values, meta)
    table = m_buf[:, 2 * pairs:, :top].astype(jnp.int32).reshape(count * per_dev)
    vmem = pl.BlockSpec(memory_space=pltpu.VMEM)
    smem = pl.BlockSpec(memory_space=pltpu.SMEM)
    anywhere = pl.BlockSpec(memory_space=pl.ANY)
    job_max = per_dev * (count - 1) if count < 2 else 2 * count
    grads = jax.ShapeDtypeStruct(queries.shape, jnp.bfloat16)
    grad_q, grad_k, grad_v = pl.pallas_call(
        functools.partial(compute_kernel, blocks, heads, top, block_len, dh, dh ** (-0.5)),
        out_shape=(grads,) * 3,
        in_specs=[smem, smem] + [vmem] * 7 + [anywhere] * 2,
        out_specs=(vmem,) * 3,
        scratch_shapes=[
            pltpu.VMEM((job_max, block_len, dh), jnp.bfloat16),
            pltpu.VMEM((job_max, block_len, dh), jnp.bfloat16),
            pltpu.VMEM((per_dev, block_len, dh), jnp.bfloat16),
            pltpu.VMEM((per_dev, block_len, dh), jnp.bfloat16),
            pltpu.VMEM((pairs, block_len, dh), jnp.float32),
            pltpu.VMEM((pairs, block_len, dh), jnp.float32),
            pltpu.SMEM((job_max,), jnp.int32),
            pltpu.SMEM((job_max,), jnp.int32),
            pltpu.SMEM((job_max,), jnp.int32),
            pltpu.SemaphoreType.DMA((2, job_max)),
            pltpu.SemaphoreType.DMA((2, per_dev)),
        ],
    )(
        table, selected.reshape(per_dev),
        queries, out_grad, keys, values, stats, meta, m_buf, a_buf, b_buf,
    )
    spread_q = lax.all_to_all(grad_q, "head", split_axis=0, concat_axis=1, tiled=True)
    return (spread_q, grad_k, grad_v)


def solution(mesh):
    placed = (P("ctx", "head"),) * 6 + (P("ctx", "head", None),)
    return jax.shard_map(
        shards,
        mesh=mesh,
        in_specs=placed,
        out_specs=(P(("ctx", "head"), None), P("ctx", "head"), P("ctx", "head")),
        check_vma=False,
    )
```

```python
import functools

import jax
import jax.numpy as jnp
from jax import lax
from jax.experimental import pallas as pl
from jax.experimental.pallas import tpu as pltpu
from jax.sharding import PartitionSpec as P

GROUP = 4
JOBS_STEP = 4
PER_PEER = 2
MESH_ID = pl.DeviceIdType.MESH
NT = (((1,), (1,)), ((), ()))
NN = (((1,), (0,)), ((), ()))


def gather_kernel(levels, q_ref, g_ref, k_ref, v_ref, m_ref, a_buf, b_buf, m_buf, send_sem, recv_sem):
    me = lax.axis_index("ctx")
    head = lax.axis_index("head")
    level = me // GROUP
    col = me % GROUP
    colx = (col + 2) % GROUP
    colc = col + 1 - 2 * (col % 2)
    down_dev = me - GROUP
    up_dev = me + GROUP
    x_dev = level * GROUP + colx
    c_dev = level * GROUP + colc
    bufs = (a_buf, b_buf, m_buf)
    down_own = (q_ref, g_ref, m_ref)
    up_own = (k_ref, v_ref, m_ref)
    has_down = level > 0
    has_up = level < levels - 1

    barrier = pltpu.get_barrier_semaphore()

    def greet(dev):
        pl.semaphore_signal(barrier, inc=1, device_id=(dev, head), device_id_type=MESH_ID)

    greet(x_dev)
    greet(c_dev)

    @pl.when(has_down)
    def _():
        greet(down_dev)

    @pl.when(has_up)
    def _():
        greet(up_dev)

    pl.semaphore_wait(barrier, 2 + has_down.astype(jnp.int32) + has_up.astype(jnp.int32))

    def copy(way, part, slot, src, dev):
        return pltpu.make_async_remote_copy(
            src_ref=src,
            dst_ref=bufs[part].at[slot],
            send_sem=send_sem.at[way, part, slot],
            recv_sem=recv_sem.at[part, slot],
            device_id=(dev, head),
            device_id_type=MESH_ID,
        )

    def push(way, slot, dev, own=None):
        for part in (2, 0, 1):
            src = bufs[part].at[slot] if own is None else own[part]
            copy(way, part, slot, src, dev).start()

    def push_part(way, part, slot, dev):
        copy(way, part, slot, bufs[part].at[slot], dev).start()

    def arrive(part, slot):
        copy(0, part, slot, bufs[part].at[slot], c_dev).wait_recv()

    def sent(way, slot, which=(0, 1, 2)):
        for part in which:
            copy(way, part, slot, bufs[part].at[slot], c_dev).wait_send()

    @pl.when(has_down)
    def _():
        push(0, me, down_dev, down_own)

    @pl.when(has_up)
    def _():
        push(3, me, up_dev, up_own)

    @pl.when(col >= 2)
    def _():
        push(1, me, x_dev, down_own)

    @pl.when(col < 2)
    def _():
        push(1, me, x_dev, up_own)

    @pl.when(col % 2 == 1)
    def _():
        push(2, me, c_dev, down_own)

    @pl.when(col % 2 == 0)
    def _():
        push(2, me, c_dev, up_own)

    def by_edge(other):
        skip_low = (level == 0) & (other == 2)
        skip_high = (level == levels - 1) & (other == levels - 3)
        return skip_low | skip_high

    def relay_low(other):
        return (level == 1) & (other == 2)

    def relay_high(other):
        return (level == levels - 2) & (other == levels - 3)

    def cross(other):
        slot = other * GROUP + colx
        for part in (2, 0, 1):
            arrive(part, slot)
            if part == 0:

                @pl.when(relay_low(other))
                def _():
                    push_part(4, part, slot, down_dev)

                @pl.when(relay_high(other))
                def _():
                    push_part(4, part, slot, up_dev)

            push_part(2, part, slot, c_dev)

    def push_across(part, other, slot):
        if part == 0:

            @pl.when(jnp.logical_not(by_edge(other)))
            def _():
                push_part(1, part, slot, x_dev)

        else:
            push_part(1, part, slot, x_dev)

    def step(dist, carry):
        high = level + dist
        low = level - dist

        @pl.when(high < levels)
        def _():
            slot = high * GROUP + col
            for part in (2, 0, 1):
                arrive(part, slot)

                @pl.when(has_down)
                def _():
                    push_part(0, part, slot, down_dev)

                push_across(part, high, slot)
                push_part(2, part, slot, c_dev)

        @pl.when(low >= 0)
        def _():
            slot = low * GROUP + col
            for part in (2, 0, 1):
                arrive(part, slot)

                @pl.when(has_up)
                def _():
                    push_part(0, part, slot, up_dev)

                push_across(part, low, slot)
                push_part(2, part, slot, c_dev)

        before = dist - 1

        @pl.when(level + before < levels)
        def _():
            cross(level + before)

        @pl.when((before > 0) & (level - before >= 0))
        def _():
            cross(level - before)

        return carry

    lax.fori_loop(1, levels + 1, step, 0)

    def finish(other, carry):
        for column in (colc, (colc + 2) % GROUP):
            for part in range(3):
                arrive(part, other * GROUP + column)
        own_slot = other * GROUP + col
        sent(1, own_slot, (1, 2))

        @pl.when(jnp.logical_not(by_edge(other)))
        def _():
            sent(1, own_slot, (0,))

        @pl.when(relay_low(other) | relay_high(other))
        def _():
            sent(4, other * GROUP + colx, (0,))

        sent(2, own_slot)
        sent(2, other * GROUP + colx)

        @pl.when(has_down & (other >= level))
        def _():
            sent(0, own_slot)

        @pl.when(has_up & (other < level))
        def _():
            sent(0, own_slot)

        @pl.when(has_up & (other == level))
        def _():
            sent(3, own_slot)

        return carry

    lax.fori_loop(0, levels, finish, 0)


def gather(queries, out_grad, keys, values, meta):
    count = lax.axis_size("ctx")
    rows = queries.shape
    anywhere = pl.BlockSpec(memory_space=pl.ANY)
    return pl.pallas_call(
        functools.partial(gather_kernel, count // GROUP),
        out_shape=(
            jax.ShapeDtypeStruct((count,) + rows, queries.dtype),
            jax.ShapeDtypeStruct((count,) + rows, queries.dtype),
            jax.ShapeDtypeStruct((count,) + meta.shape, meta.dtype),
        ),
        in_specs=[anywhere] * 5,
        out_specs=(anywhere,) * 3,
        scratch_shapes=[
            pltpu.SemaphoreType.DMA((5, 3, count)),
            pltpu.SemaphoreType.DMA((3, count)),
        ],
        compiler_params=pltpu.CompilerParams(collective_id=0, has_side_effects=True),
    )(queries, out_grad, keys, values, meta)


def dot(left, right, dims):
    return lax.dot_general(left, right, dims, preferred_element_type=jnp.float32)


def compute_kernel(
    blocks, heads, top, block_len, dh, factor,
    sel_ref,
    q_ref, g_ref, k_ref, v_ref, stat_ref, own_ref, m_buf, a_buf, b_buf,
    dq_ref, dk_ref, dv_ref,
    jq, jg, sk, sv, kacc, vacc, tab_ref, job_src, job_pair, job_key, job_sem, sel_sem, tab_sem,
):
    me = lax.axis_index("ctx")
    count = m_buf.shape[0]
    pairs = blocks * heads
    per_dev = pairs * top
    first = me * blocks

    def where_of(ref, dev, block, head):
        return ref.at[dev, pl.ds(block * block_len, block_len), pl.ds(head * dh, dh)]

    def own_of(ref, block, head):
        return ref.at[pl.ds(block * block_len, block_len), pl.ds(head * dh, dh)]

    def sel_of(entry):
        return sel_ref[entry % top, entry // top // heads, entry // top % heads]

    fetch_table = pltpu.make_async_copy(m_buf.at[:, pl.ds(2 * pairs, 1), :], tab_ref, tab_sem)
    fetch_table.start()

    for entry in range(per_dev):
        chosen = sel_of(entry)
        block, head = entry // top // heads, entry // top % heads

        @pl.when(chosen >= 0)
        def _():
            dev, inner = chosen // blocks, chosen % blocks
            pltpu.make_async_copy(where_of(a_buf, dev, inner, head), sk.at[entry], sel_sem.at[0, entry]).start()
            pltpu.make_async_copy(where_of(b_buf, dev, inner, head), sv.at[entry], sel_sem.at[1, entry]).start()

        @pl.when(chosen < 0)
        def _():
            pltpu.make_async_copy(own_of(k_ref, block, head), sk.at[entry], sel_sem.at[0, entry]).start()
            pltpu.make_async_copy(own_of(v_ref, block, head), sv.at[entry], sel_sem.at[1, entry]).start()

    def scan(dev, found):
        for entry in range(per_dev):
            chosen = tab_ref[dev, 0, entry].astype(jnp.int32)
            block, head = entry // top // heads, entry // top % heads
            hit = (chosen >= first) & (chosen < first + blocks)

            @pl.when(hit)
            def _():
                job_src[found] = dev
                job_pair[found] = entry // top
                job_key[found] = (chosen - first) * heads + head
                pltpu.make_async_copy(where_of(a_buf, dev, block, head), jq.at[found], job_sem.at[0, found]).start()
                pltpu.make_async_copy(where_of(b_buf, dev, block, head), jg.at[found], job_sem.at[1, found]).start()

            found = found + hit.astype(jnp.int32)
        return found

    fetch_table.wait()
    found = lax.fori_loop(me + 1, count, scan, jnp.int32(0))

    def owner_terms(keys, vals, qs, gs, norm, delta, causal):
        scores = dot(keys, qs, NT) * factor
        weights = jnp.exp(scores - norm)
        if causal:
            at_key = lax.broadcasted_iota(jnp.int32, scores.shape, 0)
            at_query = lax.broadcasted_iota(jnp.int32, scores.shape, 1)
            weights = jnp.where(at_key <= at_query, weights, 0.0)
        dweights = dot(vals, gs, NT)
        dscores = (weights * (dweights - delta)).astype(jnp.bfloat16)
        return dot(dscores, qs, NN) * factor, dot(weights.astype(jnp.bfloat16), gs, NN)

    def piece(ref, block, head):
        return ref[block * block_len:(block + 1) * block_len, head * dh:(head + 1) * dh]

    for pair in range(pairs):
        block, head = pair // heads, pair % heads
        part_k, part_v = owner_terms(
            piece(k_ref, block, head), piece(v_ref, block, head),
            piece(q_ref, block, head), piece(g_ref, block, head),
            own_ref[pair:pair + 1, :], own_ref[pairs + pair:pairs + pair + 1, :], True,
        )
        kacc[pair] = part_k
        vacc[pair] = part_v

    for entry in range(per_dev):
        pltpu.make_async_copy(own_of(k_ref, 0, 0), sk.at[entry], sel_sem.at[0, entry]).wait()
        pltpu.make_async_copy(own_of(v_ref, 0, 0), sv.at[entry], sel_sem.at[1, entry]).wait()
    wide = top * block_len
    for pair in range(pairs):
        block, head = pair // heads, pair % heads
        qs, gs = piece(q_ref, block, head), piece(g_ref, block, head)
        own_k, own_v = piece(k_ref, block, head), piece(v_ref, block, head)
        rows = slice(block * block_len, (block + 1) * block_len)
        norm = stat_ref[rows, head:head + 1]
        delta = stat_ref[rows, heads + head:heads + head + 1]
        far_k = sk[pair * top:(pair + 1) * top].reshape(wide, dh)
        far_v = sv[pair * top:(pair + 1) * top].reshape(wide, dh)
        weights = jnp.exp(dot(qs, own_k, NT) * factor - norm)
        at_query = lax.broadcasted_iota(jnp.int32, weights.shape, 0)
        at_key = lax.broadcasted_iota(jnp.int32, weights.shape, 1)
        weights = jnp.where(at_key <= at_query, weights, 0.0)
        near = (weights * (dot(gs, own_v, NT) - delta)).astype(jnp.bfloat16)
        weights = jnp.exp(dot(qs, far_k, NT) * factor - norm)
        far = weights * (dot(gs, far_v, NT) - delta)
        parts = []
        for turn in range(top):
            part = far[:, turn * block_len:(turn + 1) * block_len]
            parts.append(jnp.where(sel_of(pair * top + turn) >= 0, part, 0.0))
        far = jnp.concatenate(parts, axis=1).astype(jnp.bfloat16)
        total = (dot(near, own_k, NN) + dot(far, far_k, NN)) * factor
        dq_ref[rows, head * dh:(head + 1) * dh] = total.astype(dq_ref.dtype)

    def drain(job, carry):
        pltpu.make_async_copy(own_of(k_ref, 0, 0), jq.at[job], job_sem.at[0, job]).wait()
        pltpu.make_async_copy(own_of(v_ref, 0, 0), jg.at[job], job_sem.at[1, job]).wait()
        return carry

    lax.fori_loop(0, found, drain, 0)

    def turn(step, carry):
        results = []
        for lane in range(JOBS_STEP):
            job = step * JOBS_STEP + lane
            live = job < found
            job = jnp.minimum(job, found - 1)
            key = job_key[job]
            src, pair = job_src[job], job_pair[job]
            block, head = key // heads, key % heads
            rows = pl.ds(pl.multiple_of(block * block_len, block_len), block_len)
            cols = pl.ds(pl.multiple_of(head * dh, dh), dh)
            part_k, part_v = owner_terms(
                k_ref[rows, cols], v_ref[rows, cols], jq[job], jg[job],
                m_buf[src, pl.ds(pair, 1), :], m_buf[src, pl.ds(pairs + pair, 1), :], False,
            )
            results.append((key, jnp.where(live, part_k, 0.0), jnp.where(live, part_v, 0.0)))
        for key, part_k, part_v in results:
            kacc[key] += part_k
            vacc[key] += part_v
        return carry

    lax.fori_loop(0, (found + JOBS_STEP - 1) // JOBS_STEP, turn, 0)
    for pair in range(pairs):
        block, head = pair // heads, pair % heads
        rows = slice(block * block_len, (block + 1) * block_len)
        dk_ref[rows, head * dh:(head + 1) * dh] = kacc[pair].astype(dk_ref.dtype)
        dv_ref[rows, head * dh:(head + 1) * dh] = vacc[pair].astype(dv_ref.dtype)


def prep_kernel(blocks, heads, top, block_len, dh, sel_ref, g_ref, o_ref, n_ref, stat_ref, meta_ref):
    pairs = blocks * heads
    lanes = lax.broadcasted_iota(jnp.int32, (block_len, block_len), 1)
    for block in range(blocks):
        rows = slice(block * block_len, (block + 1) * block_len)
        table = jnp.zeros((block_len, block_len), jnp.float32)
        for head in range(heads):
            cols = slice(head * dh, (head + 1) * dh)
            terms = g_ref[rows, cols].astype(jnp.float32) * o_ref[rows, cols].astype(jnp.float32)
            delta = jnp.sum(terms, axis=1, keepdims=True)
            table = jnp.where(lanes == heads + head, delta, table)
        norms = n_ref[:, rows]
        spread = jnp.concatenate([norms, jnp.zeros((block_len - heads, block_len), jnp.float32)], axis=0)
        stat_ref[rows, :] = (table + jnp.transpose(spread))[:, :2 * heads]
        turned = jnp.transpose(table)
        meta_ref[block * heads:(block + 1) * heads, :] = norms
        meta_ref[pairs + block * heads:pairs + (block + 1) * heads, :] = turned[heads:2 * heads]
    lane = lax.broadcasted_iota(jnp.int32, (8, block_len), 1)
    chosen = jnp.zeros((8, block_len), jnp.int32)
    for entry in range(pairs * top):
        value = sel_ref[entry % top, entry // top // heads, entry // top % heads]
        chosen = jnp.where(lane == entry, value, chosen)
    meta_ref[2 * pairs:2 * pairs + 8, :] = chosen.astype(jnp.float32)


def shards(queries, keys, values, out_grad, outputs, log_norms, selected):
    blocks, heads, top = selected.shape
    row_count, width = queries.shape
    dh = width // heads
    block_len = row_count // blocks
    pairs = blocks * heads
    count = lax.axis_size("ctx")
    per_dev = pairs * top
    vmem = pl.BlockSpec(memory_space=pltpu.VMEM)
    smem = pl.BlockSpec(memory_space=pltpu.SMEM)
    anywhere = pl.BlockSpec(memory_space=pl.ANY)
    chosen = jnp.transpose(selected, (2, 0, 1))
    stats, meta = pl.pallas_call(
        functools.partial(prep_kernel, blocks, heads, top, block_len, dh),
        out_shape=(
            jax.ShapeDtypeStruct((row_count, 2 * heads), jnp.float32),
            jax.ShapeDtypeStruct((2 * pairs + 8, block_len), jnp.float32),
        ),
        in_specs=[smem] + [vmem] * 3,
        out_specs=(vmem,) * 2,
    )(chosen, out_grad, outputs, jnp.transpose(log_norms))
    a_buf, b_buf, m_buf = gather(queries, out_grad, keys, values, meta)
    job_max = PER_PEER * count
    grads = jax.ShapeDtypeStruct(queries.shape, jnp.bfloat16)
    grad_q, grad_k, grad_v = pl.pallas_call(
        functools.partial(compute_kernel, blocks, heads, top, block_len, dh, dh ** (-0.5)),
        out_shape=(grads,) * 3,
        in_specs=[smem] + [vmem] * 7 + [anywhere] * 2,
        out_specs=(vmem,) * 3,
        scratch_shapes=[
            pltpu.VMEM((job_max, block_len, dh), jnp.bfloat16),
            pltpu.VMEM((job_max, block_len, dh), jnp.bfloat16),
            pltpu.VMEM((per_dev, block_len, dh), jnp.bfloat16),
            pltpu.VMEM((per_dev, block_len, dh), jnp.bfloat16),
            pltpu.VMEM((pairs, block_len, dh), jnp.float32),
            pltpu.VMEM((pairs, block_len, dh), jnp.float32),
            pltpu.SMEM((count, 1, block_len), jnp.float32),
            pltpu.SMEM((job_max,), jnp.int32),
            pltpu.SMEM((job_max,), jnp.int32),
            pltpu.SMEM((job_max,), jnp.int32),
            pltpu.SemaphoreType.DMA((2, job_max)),
            pltpu.SemaphoreType.DMA((2, per_dev)),
            pltpu.SemaphoreType.DMA,
        ],
    )(
        chosen,
        queries, out_grad, keys, values, stats, meta, m_buf, a_buf, b_buf,
    )
    spread_q = lax.all_to_all(grad_q, "head", split_axis=0, concat_axis=1, tiled=True)
    return (spread_q, grad_k, grad_v)


def solution(mesh):
    placed = (P("ctx", "head"),) * 6 + (P("ctx", "head", None),)
    return jax.shard_map(
        shards,
        mesh=mesh,
        in_specs=placed,
        out_specs=(P(("ctx", "head"), None), P("ctx", "head"), P("ctx", "head")),
        check_vma=False,
    )
```

```python
import functools

import jax
import jax.numpy as jnp
from jax import lax
from jax.experimental import pallas as pl
from jax.experimental.pallas import tpu as pltpu
from jax.sharding import PartitionSpec as P

GROUP = 4
JOBS_STEP = 4
PER_PEER = 2
MESH_ID = pl.DeviceIdType.MESH
NT = (((1,), (1,)), ((), ()))
NN = (((1,), (0,)), ((), ()))


def gather_kernel(levels, q_ref, g_ref, k_ref, v_ref, m_ref, a_buf, b_buf, m_buf, send_sem, recv_sem):
    me = lax.axis_index("ctx")
    head = lax.axis_index("head")
    level = me // GROUP
    col = me % GROUP
    colx = (col + 2) % GROUP
    colc = col + 1 - 2 * (col % 2)
    down_dev = me - GROUP
    up_dev = me + GROUP
    x_dev = level * GROUP + colx
    c_dev = level * GROUP + colc
    bufs = (a_buf, b_buf, m_buf)
    down_own = (q_ref, g_ref, m_ref)
    up_own = (k_ref, v_ref, m_ref)
    has_down = level > 0
    has_up = level < levels - 1

    barrier = pltpu.get_barrier_semaphore()

    def greet(dev):
        pl.semaphore_signal(barrier, inc=1, device_id=(dev, head), device_id_type=MESH_ID)

    greet(x_dev)
    greet(c_dev)

    @pl.when(has_down)
    def _():
        greet(down_dev)

    @pl.when(has_up)
    def _():
        greet(up_dev)

    pl.semaphore_wait(barrier, 2 + has_down.astype(jnp.int32) + has_up.astype(jnp.int32))

    def copy(way, part, slot, src, dev):
        return pltpu.make_async_remote_copy(
            src_ref=src,
            dst_ref=bufs[part].at[slot],
            send_sem=send_sem.at[way, part, slot],
            recv_sem=recv_sem.at[part, slot],
            device_id=(dev, head),
            device_id_type=MESH_ID,
        )

    def push(way, slot, dev, own=None):
        for part in (2, 0, 1):
            src = bufs[part].at[slot] if own is None else own[part]
            copy(way, part, slot, src, dev).start()

    def push_part(way, part, slot, dev):
        copy(way, part, slot, bufs[part].at[slot], dev).start()

    def arrive(part, slot):
        copy(0, part, slot, bufs[part].at[slot], c_dev).wait_recv()

    def sent(way, slot, which=(0, 1, 2)):
        for part in which:
            copy(way, part, slot, bufs[part].at[slot], c_dev).wait_send()

    @pl.when(has_down)
    def _():
        push(0, me, down_dev, down_own)

    @pl.when(has_up)
    def _():
        push(3, me, up_dev, up_own)

    @pl.when(col >= 2)
    def _():
        push(1, me, x_dev, down_own)

    @pl.when(col < 2)
    def _():
        push(1, me, x_dev, up_own)

    @pl.when(col % 2 == 1)
    def _():
        push(2, me, c_dev, down_own)

    @pl.when(col % 2 == 0)
    def _():
        push(2, me, c_dev, up_own)

    def by_edge(other):
        skip_low = (level == 0) & (other == 2)
        skip_high = (level == levels - 1) & (other == levels - 3)
        return skip_low | skip_high

    def relay_low(other):
        return (level == 1) & (other == 2)

    def relay_high(other):
        return (level == levels - 2) & (other == levels - 3)

    def cross(other):
        slot = other * GROUP + colx
        for part in (2, 0, 1):
            arrive(part, slot)
            if part == 0:

                @pl.when(relay_low(other))
                def _():
                    push_part(4, part, slot, down_dev)

                @pl.when(relay_high(other))
                def _():
                    push_part(4, part, slot, up_dev)

            push_part(2, part, slot, c_dev)

    def push_across(part, other, slot):
        if part == 0:

            @pl.when(jnp.logical_not(by_edge(other)))
            def _():
                push_part(1, part, slot, x_dev)

        else:
            push_part(1, part, slot, x_dev)

    def step(dist, carry):
        high = level + dist
        low = level - dist

        @pl.when(high < levels)
        def _():
            slot = high * GROUP + col
            for part in (2, 0, 1):
                arrive(part, slot)

                @pl.when(has_down)
                def _():
                    push_part(0, part, slot, down_dev)

                push_across(part, high, slot)
                push_part(2, part, slot, c_dev)

        @pl.when(low >= 0)
        def _():
            slot = low * GROUP + col
            for part in (2, 0, 1):
                arrive(part, slot)

                @pl.when(has_up)
                def _():
                    push_part(0, part, slot, up_dev)

                push_across(part, low, slot)
                push_part(2, part, slot, c_dev)

        before = dist - 1

        @pl.when(level + before < levels)
        def _():
            cross(level + before)

        @pl.when((before > 0) & (level - before >= 0))
        def _():
            cross(level - before)

        return carry

    lax.fori_loop(1, levels + 1, step, 0)

    def finish(other, carry):
        for column in (colc, (colc + 2) % GROUP):
            for part in range(3):
                arrive(part, other * GROUP + column)
        own_slot = other * GROUP + col
        sent(1, own_slot, (1, 2))

        @pl.when(jnp.logical_not(by_edge(other)))
        def _():
            sent(1, own_slot, (0,))

        @pl.when(relay_low(other) | relay_high(other))
        def _():
            sent(4, other * GROUP + colx, (0,))

        sent(2, own_slot)
        sent(2, other * GROUP + colx)

        @pl.when(has_down & (other >= level))
        def _():
            sent(0, own_slot)

        @pl.when(has_up & (other < level))
        def _():
            sent(0, own_slot)

        @pl.when(has_up & (other == level))
        def _():
            sent(3, own_slot)

        return carry

    lax.fori_loop(0, levels, finish, 0)


def gather(queries, out_grad, keys, values, meta):
    count = lax.axis_size("ctx")
    rows = queries.shape
    anywhere = pl.BlockSpec(memory_space=pl.ANY)
    return pl.pallas_call(
        functools.partial(gather_kernel, count // GROUP),
        out_shape=(
            jax.ShapeDtypeStruct((count,) + rows, queries.dtype),
            jax.ShapeDtypeStruct((count,) + rows, queries.dtype),
            jax.ShapeDtypeStruct((count,) + meta.shape, meta.dtype),
        ),
        in_specs=[anywhere] * 5,
        out_specs=(anywhere,) * 3,
        scratch_shapes=[
            pltpu.SemaphoreType.DMA((5, 3, count)),
            pltpu.SemaphoreType.DMA((3, count)),
        ],
        compiler_params=pltpu.CompilerParams(collective_id=0, has_side_effects=True),
    )(queries, out_grad, keys, values, meta)


def dot(left, right, dims):
    return lax.dot_general(left, right, dims, preferred_element_type=jnp.float32)


def piece(ref, block, head, block_len, dh):
    return ref[block * block_len:(block + 1) * block_len, head * dh:(head + 1) * dh]


def view(ref, block, head, block_len, dh):
    return ref.at[pl.ds(block * block_len, block_len), pl.ds(head * dh, dh)]


def far_view(ref, dev, block, head, block_len, dh):
    return ref.at[dev, pl.ds(block * block_len, block_len), pl.ds(head * dh, dh)]


def query_kernel(
    blocks, heads, top, block_len, dh, factor,
    sel_ref, q_ref, g_ref, k_ref, v_ref, stat_ref, a_buf, b_buf, dq_ref, sk, sv, sel_sem,
):
    chunks, size = dq_ref.shape[0], dq_ref.shape[1]
    mine = lax.axis_index("head")
    pairs = blocks * heads
    per_dev = pairs * top
    place = (block_len, dh)

    def sel_of(entry):
        return sel_ref[entry % top, entry // top // heads, entry // top % heads]

    for entry in range(per_dev):
        chosen = sel_of(entry)
        block, head = entry // top // heads, entry // top % heads

        @pl.when(chosen >= 0)
        def _():
            dev, inner = chosen // blocks, chosen % blocks
            pltpu.make_async_copy(far_view(a_buf, dev, inner, head, *place), sk.at[entry], sel_sem.at[0, entry]).start()
            pltpu.make_async_copy(far_view(b_buf, dev, inner, head, *place), sv.at[entry], sel_sem.at[1, entry]).start()

        @pl.when(chosen < 0)
        def _():
            pltpu.make_async_copy(view(k_ref, block, head, *place), sk.at[entry], sel_sem.at[0, entry]).start()
            pltpu.make_async_copy(view(v_ref, block, head, *place), sv.at[entry], sel_sem.at[1, entry]).start()

    for entry in range(per_dev):
        pltpu.make_async_copy(view(k_ref, 0, 0, *place), sk.at[entry], sel_sem.at[0, entry]).wait()
        pltpu.make_async_copy(view(v_ref, 0, 0, *place), sv.at[entry], sel_sem.at[1, entry]).wait()
    wide = top * block_len
    for pair in range(pairs):
        block, head = pair // heads, pair % heads
        qs, gs = piece(q_ref, block, head, *place), piece(g_ref, block, head, *place)
        own_k, own_v = piece(k_ref, block, head, *place), piece(v_ref, block, head, *place)
        rows = slice(block * block_len, (block + 1) * block_len)
        norm = stat_ref[rows, head:head + 1]
        delta = stat_ref[rows, heads + head:heads + head + 1]
        far_k = sk[pair * top:(pair + 1) * top].reshape(wide, dh)
        far_v = sv[pair * top:(pair + 1) * top].reshape(wide, dh)
        weights = jnp.exp(dot(qs, own_k, NT) * factor - norm)
        at_query = lax.broadcasted_iota(jnp.int32, weights.shape, 0)
        at_key = lax.broadcasted_iota(jnp.int32, weights.shape, 1)
        weights = jnp.where(at_key <= at_query, weights, 0.0)
        near = (weights * (dot(gs, own_v, NT) - delta)).astype(jnp.bfloat16)
        weights = jnp.exp(dot(qs, far_k, NT) * factor - norm)
        far = weights * (dot(gs, far_v, NT) - delta)
        parts = []
        for turn in range(top):
            part = far[:, turn * block_len:(turn + 1) * block_len]
            parts.append(jnp.where(sel_of(pair * top + turn) >= 0, part, 0.0))
        far = jnp.concatenate(parts, axis=1).astype(jnp.bfloat16)
        total = ((dot(near, own_k, NN) + dot(far, far_k, NN)) * factor).astype(dq_ref.dtype)
        step = min(size, block_len)
        for start in range(0, block_len, step):
            row = block * block_len + start
            chunk = (row // size + chunks - mine) % chunks
            dq_ref[chunk, row % size:row % size + step, head * dh:(head + 1) * dh] = total[start:start + step]


def owner_kernel(
    blocks, heads, block_len, dh, factor,
    q_ref, g_ref, k_ref, v_ref, own_ref, m_buf, a_buf, b_buf,
    dk_ref, dv_ref,
    jq, jg, kacc, vacc, tab_ref, job_src, job_pair, job_key, job_sem, tab_sem,
):
    me = lax.axis_index("ctx")
    count = m_buf.shape[0]
    pairs = blocks * heads
    place = (block_len, dh)

    fetch_table = pltpu.make_async_copy(m_buf.at[:, pl.ds(2 * pairs, PER_PEER), :], tab_ref, tab_sem)
    fetch_table.start()
    fetch_table.wait()

    def scan(dev, found):
        for rank in range(PER_PEER):
            code = tab_ref[dev, rank, me].astype(jnp.int32)
            pair = code // blocks
            block, head = pair // heads, pair % heads

            @pl.when(code >= 0)
            def _():
                job_src[found] = dev
                job_pair[found] = pair
                job_key[found] = (code % blocks) * heads + head
                row = pl.multiple_of(block * block_len, block_len)
                col = pl.multiple_of(head * dh, dh)
                spot = (dev, pl.ds(row, block_len), pl.ds(col, dh))
                pltpu.make_async_copy(a_buf.at[spot], jq.at[found], job_sem.at[0, found]).start()
                pltpu.make_async_copy(b_buf.at[spot], jg.at[found], job_sem.at[1, found]).start()

            found = found + (code >= 0).astype(jnp.int32)
        return found

    found = lax.fori_loop(me + 1, count, scan, jnp.int32(0))

    def owner_terms(keys, vals, qs, gs, norm, delta, causal):
        scores = dot(keys, qs, NT) * factor
        weights = jnp.exp(scores - norm)
        if causal:
            at_key = lax.broadcasted_iota(jnp.int32, scores.shape, 0)
            at_query = lax.broadcasted_iota(jnp.int32, scores.shape, 1)
            weights = jnp.where(at_key <= at_query, weights, 0.0)
        dweights = dot(vals, gs, NT)
        dscores = (weights * (dweights - delta)).astype(jnp.bfloat16)
        return dot(dscores, qs, NN) * factor, dot(weights.astype(jnp.bfloat16), gs, NN)

    for pair in range(pairs):
        block, head = pair // heads, pair % heads
        part_k, part_v = owner_terms(
            piece(k_ref, block, head, *place), piece(v_ref, block, head, *place),
            piece(q_ref, block, head, *place), piece(g_ref, block, head, *place),
            own_ref[pair:pair + 1, :], own_ref[pairs + pair:pairs + pair + 1, :], True,
        )
        kacc[pair] = part_k
        vacc[pair] = part_v

    def drain(job, carry):
        pltpu.make_async_copy(view(k_ref, 0, 0, *place), jq.at[job], job_sem.at[0, job]).wait()
        pltpu.make_async_copy(view(v_ref, 0, 0, *place), jg.at[job], job_sem.at[1, job]).wait()
        return carry

    lax.fori_loop(0, found, drain, 0)

    def turn(step, carry):
        results = []
        for lane in range(JOBS_STEP):
            job = step * JOBS_STEP + lane
            live = job < found
            job = jnp.minimum(job, found - 1)
            key = job_key[job]
            src, pair = job_src[job], job_pair[job]
            block, head = key // heads, key % heads
            rows = pl.ds(pl.multiple_of(block * block_len, block_len), block_len)
            cols = pl.ds(pl.multiple_of(head * dh, dh), dh)
            part_k, part_v = owner_terms(
                k_ref[rows, cols], v_ref[rows, cols], jq[job], jg[job],
                m_buf[src, pl.ds(pair, 1), :], m_buf[src, pl.ds(pairs + pair, 1), :], False,
            )
            results.append((key, jnp.where(live, part_k, 0.0), jnp.where(live, part_v, 0.0)))
        for key, part_k, part_v in results:
            kacc[key] += part_k
            vacc[key] += part_v
        return carry

    lax.fori_loop(0, (found + JOBS_STEP - 1) // JOBS_STEP, turn, 0)
    for pair in range(pairs):
        block, head = pair // heads, pair % heads
        rows = slice(block * block_len, (block + 1) * block_len)
        dk_ref[rows, head * dh:(head + 1) * dh] = kacc[pair].astype(dk_ref.dtype)
        dv_ref[rows, head * dh:(head + 1) * dh] = vacc[pair].astype(dv_ref.dtype)


def join_kernel(chunk_ref, *refs):
    moved, out_ref = refs[:-1], refs[-1]
    chunks, size, width = chunk_ref.shape
    mine = lax.axis_index("head")
    for shift in range(chunks):
        source = (mine + chunks - shift) % chunks
        cols = pl.ds(pl.multiple_of(source * width, width), width)
        out_ref[:, cols] = chunk_ref[0] if shift == 0 else moved[shift - 1][...]


def prep_kernel(blocks, heads, top, block_len, dh, sel_ref, g_ref, o_ref, n_ref, stat_ref, meta_ref):
    pairs = blocks * heads
    lanes = lax.broadcasted_iota(jnp.int32, (block_len, block_len), 1)
    for block in range(blocks):
        rows = slice(block * block_len, (block + 1) * block_len)
        table = jnp.zeros((block_len, block_len), jnp.float32)
        for head in range(heads):
            cols = slice(head * dh, (head + 1) * dh)
            terms = g_ref[rows, cols].astype(jnp.float32) * o_ref[rows, cols].astype(jnp.float32)
            delta = jnp.sum(terms, axis=1, keepdims=True)
            table = jnp.where(lanes == heads + head, delta, table)
        norms = n_ref[:, rows]
        spread = jnp.concatenate([norms, jnp.zeros((block_len - heads, block_len), jnp.float32)], axis=0)
        stat_ref[rows, :] = (table + jnp.transpose(spread))[:, :2 * heads]
        turned = jnp.transpose(table)
        meta_ref[block * heads:(block + 1) * heads, :] = norms
        meta_ref[pairs + block * heads:pairs + (block + 1) * heads, :] = turned[heads:2 * heads]
    lane = lax.broadcasted_iota(jnp.int32, (8, block_len), 1)
    slots = [jnp.full((8, block_len), -1, jnp.int32) for _ in range(PER_PEER)]
    for entry in range(pairs * top):
        value = sel_ref[entry % top, entry // top // heads, entry // top % heads]
        owner = jnp.where(value >= 0, value // blocks, -1)
        code = (entry // top) * blocks + value % blocks
        here = lane == owner
        for rank in range(PER_PEER):
            free = slots[rank] < 0
            slots[rank] = jnp.where(here & free, code, slots[rank])
            here = here & jnp.logical_not(free)
    row = lax.broadcasted_iota(jnp.int32, (8, block_len), 0)
    table = jnp.zeros((8, block_len), jnp.int32)
    for rank in range(PER_PEER):
        table = jnp.where(row == rank, slots[rank], table)
    meta_ref[2 * pairs:2 * pairs + 8, :] = table.astype(jnp.float32)


def shards(queries, keys, values, out_grad, outputs, log_norms, selected):
    blocks, heads, top = selected.shape
    row_count, width = queries.shape
    dh = width // heads
    block_len = row_count // blocks
    pairs = blocks * heads
    count = lax.axis_size("ctx")
    per_dev = pairs * top
    vmem = pl.BlockSpec(memory_space=pltpu.VMEM)
    smem = pl.BlockSpec(memory_space=pltpu.SMEM)
    anywhere = pl.BlockSpec(memory_space=pl.ANY)
    chosen = jnp.transpose(selected, (2, 0, 1))
    stats, meta = pl.pallas_call(
        functools.partial(prep_kernel, blocks, heads, top, block_len, dh),
        out_shape=(
            jax.ShapeDtypeStruct((row_count, 2 * heads), jnp.float32),
            jax.ShapeDtypeStruct((2 * pairs + 8, block_len), jnp.float32),
        ),
        in_specs=[smem] + [vmem] * 3,
        out_specs=(vmem,) * 2,
    )(chosen, out_grad, outputs, jnp.transpose(log_norms))
    a_buf, b_buf, m_buf = gather(queries, out_grad, keys, values, meta)
    job_max = PER_PEER * count
    chunks = lax.axis_size("head")
    factor = dh ** (-0.5)
    spare = pltpu.VMEM((per_dev, block_len, dh), jnp.bfloat16)
    chunk_q = pl.pallas_call(
        functools.partial(query_kernel, blocks, heads, top, block_len, dh, factor),
        out_shape=jax.ShapeDtypeStruct((chunks, row_count // chunks, width), jnp.bfloat16),
        in_specs=[smem] + [vmem] * 5 + [anywhere] * 2,
        out_specs=vmem,
        scratch_shapes=[spare, spare, pltpu.SemaphoreType.DMA((2, per_dev))],
        cost_estimate=pl.CostEstimate(flops=10**9, bytes_accessed=4 * 10**6, transcendentals=10**6),
    )(chosen, queries, out_grad, keys, values, stats, a_buf, b_buf)
    moved = []
    for shift in range(1, chunks):
        ring = [(at, (at + shift) % chunks) for at in range(chunks)]
        moved.append(lax.ppermute(chunk_q[shift], "head", ring))
    grads = jax.ShapeDtypeStruct(queries.shape, jnp.bfloat16)
    jobs = pltpu.VMEM((job_max, block_len, dh), jnp.bfloat16)
    sums = pltpu.VMEM((pairs, block_len, dh), jnp.float32)
    grad_k, grad_v = pl.pallas_call(
        functools.partial(owner_kernel, blocks, heads, block_len, dh, factor),
        out_shape=(grads,) * 2,
        in_specs=[vmem] * 6 + [anywhere] * 2,
        out_specs=(vmem,) * 2,
        scratch_shapes=[
            jobs, jobs, sums, sums,
            pltpu.SMEM((count, PER_PEER, block_len), jnp.float32),
            pltpu.SMEM((job_max,), jnp.int32),
            pltpu.SMEM((job_max,), jnp.int32),
            pltpu.SMEM((job_max,), jnp.int32),
            pltpu.SemaphoreType.DMA((2, job_max)),
            pltpu.SemaphoreType.DMA,
        ],
        cost_estimate=pl.CostEstimate(flops=4 * 10**9, bytes_accessed=8 * 10**6, transcendentals=10**6),
    )(queries, out_grad, keys, values, meta, m_buf, a_buf, b_buf)
    spread_q = pl.pallas_call(
        join_kernel,
        out_shape=jax.ShapeDtypeStruct((row_count // chunks, chunks * width), jnp.bfloat16),
        in_specs=[vmem] * chunks,
        out_specs=vmem,
    )(chunk_q, *moved)
    return (spread_q, grad_k, grad_v)


def solution(mesh):
    placed = (P("ctx", "head"),) * 6 + (P("ctx", "head", None),)
    return jax.shard_map(
        shards,
        mesh=mesh,
        in_specs=placed,
        out_specs=(P(("ctx", "head"), None), P("ctx", "head"), P("ctx", "head")),
        check_vma=False,
    )
```

```python
import functools

import jax
import jax.numpy as jnp
from jax import lax
from jax.experimental import pallas as pl
from jax.experimental.pallas import tpu as pltpu
from jax.sharding import PartitionSpec as P

GROUP = 4
JOBS_STEP = 4
PER_PEER = 2
MESH_ID = pl.DeviceIdType.MESH
NT = (((1,), (1,)), ((), ()))
NN = (((1,), (0,)), ((), ()))


def gather_kernel(levels, q_ref, g_ref, k_ref, v_ref, m_ref, a_buf, b_buf, m_buf, send_sem, recv_sem):
    me = lax.axis_index("ctx")
    head = lax.axis_index("head")
    level = me // GROUP
    col = me % GROUP
    colx = (col + 2) % GROUP
    colc = col + 1 - 2 * (col % 2)
    down_dev = me - GROUP
    up_dev = me + GROUP
    x_dev = level * GROUP + colx
    c_dev = level * GROUP + colc
    bufs = (a_buf, b_buf, m_buf)
    down_own = (q_ref, g_ref, m_ref)
    up_own = (k_ref, v_ref, m_ref)
    has_down = level > 0
    has_up = level < levels - 1

    barrier = pltpu.get_barrier_semaphore()

    def greet(dev):
        pl.semaphore_signal(barrier, inc=1, device_id=(dev, head), device_id_type=MESH_ID)

    greet(x_dev)
    greet(c_dev)

    @pl.when(has_down)
    def _():
        greet(down_dev)

    @pl.when(has_up)
    def _():
        greet(up_dev)

    pl.semaphore_wait(barrier, 2 + has_down.astype(jnp.int32) + has_up.astype(jnp.int32))

    def copy(way, part, slot, src, dev):
        return pltpu.make_async_remote_copy(
            src_ref=src,
            dst_ref=bufs[part].at[slot],
            send_sem=send_sem.at[way, part, slot],
            recv_sem=recv_sem.at[part, slot],
            device_id=(dev, head),
            device_id_type=MESH_ID,
        )

    def push(way, slot, dev, own=None):
        for part in (2, 0, 1):
            src = bufs[part].at[slot] if own is None else own[part]
            copy(way, part, slot, src, dev).start()

    def push_part(way, part, slot, dev):
        copy(way, part, slot, bufs[part].at[slot], dev).start()

    def arrive(part, slot):
        copy(0, part, slot, bufs[part].at[slot], c_dev).wait_recv()

    def sent(way, slot, which=(0, 1, 2)):
        for part in which:
            copy(way, part, slot, bufs[part].at[slot], c_dev).wait_send()

    @pl.when(has_down)
    def _():
        push(0, me, down_dev, down_own)

    @pl.when(has_up)
    def _():
        push(3, me, up_dev, up_own)

    @pl.when(col >= 2)
    def _():
        push(1, me, x_dev, down_own)

    @pl.when(col < 2)
    def _():
        push(1, me, x_dev, up_own)

    @pl.when(col % 2 == 1)
    def _():
        push(2, me, c_dev, down_own)

    @pl.when(col % 2 == 0)
    def _():
        push(2, me, c_dev, up_own)

    def by_edge(other):
        to_low = (other == level + 1) | ((level == levels - 1) & (other == levels - 3))
        to_high = (other == level - 1) | ((level == 0) & (other == 2))
        return ((col >= 2) & to_low) | ((col < 2) & to_high)

    def relay_low(other):
        near = (other == level) & (col < 2) & has_down
        return near | ((level == 1) & (other == 2) & (col >= 2))

    def relay_high(other):
        near = (other == level) & (col >= 2) & has_up
        return near | ((level == levels - 2) & (other == levels - 3) & (col < 2))

    def cross(other):
        slot = other * GROUP + colx
        for part in (2, 0, 1):
            arrive(part, slot)
            if part == 0:

                @pl.when(relay_low(other))
                def _():
                    push_part(4, part, slot, down_dev)

                @pl.when(relay_high(other))
                def _():
                    push_part(4, part, slot, up_dev)

            push_part(2, part, slot, c_dev)

    def push_across(part, other, slot):
        if part == 0:

            @pl.when(jnp.logical_not(by_edge(other)))
            def _():
                push_part(1, part, slot, x_dev)

        else:
            push_part(1, part, slot, x_dev)

    def step(dist, carry):
        high = level + dist
        low = level - dist

        @pl.when(high < levels)
        def _():
            slot = high * GROUP + col
            for part in (2, 0, 1):
                arrive(part, slot)

                @pl.when(has_down)
                def _():
                    push_part(0, part, slot, down_dev)

                push_across(part, high, slot)
                push_part(2, part, slot, c_dev)

        @pl.when(low >= 0)
        def _():
            slot = low * GROUP + col
            for part in (2, 0, 1):
                arrive(part, slot)

                @pl.when(has_up)
                def _():
                    push_part(0, part, slot, up_dev)

                push_across(part, low, slot)
                push_part(2, part, slot, c_dev)

        before = dist - 1

        @pl.when(level + before < levels)
        def _():
            cross(level + before)

        @pl.when((before > 0) & (level - before >= 0))
        def _():
            cross(level - before)

        return carry

    lax.fori_loop(1, levels + 1, step, 0)

    def finish(other, carry):
        for column in (colc, (colc + 2) % GROUP):
            for part in range(3):
                arrive(part, other * GROUP + column)
        own_slot = other * GROUP + col
        sent(1, own_slot, (1, 2))

        @pl.when(jnp.logical_not(by_edge(other)))
        def _():
            sent(1, own_slot, (0,))

        @pl.when(relay_low(other) | relay_high(other))
        def _():
            sent(4, other * GROUP + colx, (0,))

        sent(2, own_slot)
        sent(2, other * GROUP + colx)

        @pl.when(has_down & (other >= level))
        def _():
            sent(0, own_slot)

        @pl.when(has_up & (other < level))
        def _():
            sent(0, own_slot)

        @pl.when(has_up & (other == level))
        def _():
            sent(3, own_slot)

        return carry

    lax.fori_loop(0, levels, finish, 0)


def gather(queries, out_grad, keys, values, meta):
    count = lax.axis_size("ctx")
    rows = queries.shape
    anywhere = pl.BlockSpec(memory_space=pl.ANY)
    return pl.pallas_call(
        functools.partial(gather_kernel, count // GROUP),
        out_shape=(
            jax.ShapeDtypeStruct((count,) + rows, queries.dtype),
            jax.ShapeDtypeStruct((count,) + rows, queries.dtype),
            jax.ShapeDtypeStruct((count,) + meta.shape, meta.dtype),
        ),
        in_specs=[anywhere] * 5,
        out_specs=(anywhere,) * 3,
        scratch_shapes=[
            pltpu.SemaphoreType.DMA((5, 3, count)),
            pltpu.SemaphoreType.DMA((3, count)),
        ],
        compiler_params=pltpu.CompilerParams(collective_id=0, has_side_effects=True),
    )(queries, out_grad, keys, values, meta)


def dot(left, right, dims):
    return lax.dot_general(left, right, dims, preferred_element_type=jnp.float32)


def piece(ref, block, head, block_len, dh):
    return ref[block * block_len:(block + 1) * block_len, head * dh:(head + 1) * dh]


def view(ref, block, head, block_len, dh):
    return ref.at[pl.ds(block * block_len, block_len), pl.ds(head * dh, dh)]


def far_view(ref, dev, block, head, block_len, dh):
    return ref.at[dev, pl.ds(block * block_len, block_len), pl.ds(head * dh, dh)]


def query_kernel(
    blocks, heads, top, block_len, dh, factor,
    sel_ref, q_ref, g_ref, k_ref, v_ref, stat_ref, a_buf, b_buf, dq_ref, sk, sv, sel_sem,
):
    chunks, size = dq_ref.shape[0], dq_ref.shape[1]
    mine = lax.axis_index("head")
    pairs = blocks * heads
    per_dev = pairs * top
    place = (block_len, dh)

    def sel_of(entry):
        return sel_ref[entry % top, entry // top // heads, entry // top % heads]

    for entry in range(per_dev):
        chosen = sel_of(entry)
        block, head = entry // top // heads, entry // top % heads

        @pl.when(chosen >= 0)
        def _():
            dev, inner = chosen // blocks, chosen % blocks
            pltpu.make_async_copy(far_view(a_buf, dev, inner, head, *place), sk.at[entry], sel_sem.at[0, entry]).start()
            pltpu.make_async_copy(far_view(b_buf, dev, inner, head, *place), sv.at[entry], sel_sem.at[1, entry]).start()

        @pl.when(chosen < 0)
        def _():
            pltpu.make_async_copy(view(k_ref, block, head, *place), sk.at[entry], sel_sem.at[0, entry]).start()
            pltpu.make_async_copy(view(v_ref, block, head, *place), sv.at[entry], sel_sem.at[1, entry]).start()

    for entry in range(per_dev):
        pltpu.make_async_copy(view(k_ref, 0, 0, *place), sk.at[entry], sel_sem.at[0, entry]).wait()
        pltpu.make_async_copy(view(v_ref, 0, 0, *place), sv.at[entry], sel_sem.at[1, entry]).wait()
    wide = top * block_len
    for pair in range(pairs):
        block, head = pair // heads, pair % heads
        qs, gs = piece(q_ref, block, head, *place), piece(g_ref, block, head, *place)
        own_k, own_v = piece(k_ref, block, head, *place), piece(v_ref, block, head, *place)
        rows = slice(block * block_len, (block + 1) * block_len)
        norm = stat_ref[rows, head:head + 1]
        delta = stat_ref[rows, heads + head:heads + head + 1]
        far_k = sk[pair * top:(pair + 1) * top].reshape(wide, dh)
        far_v = sv[pair * top:(pair + 1) * top].reshape(wide, dh)
        weights = jnp.exp(dot(qs, own_k, NT) * factor - norm)
        at_query = lax.broadcasted_iota(jnp.int32, weights.shape, 0)
        at_key = lax.broadcasted_iota(jnp.int32, weights.shape, 1)
        weights = jnp.where(at_key <= at_query, weights, 0.0)
        near = (weights * (dot(gs, own_v, NT) - delta)).astype(jnp.bfloat16)
        weights = jnp.exp(dot(qs, far_k, NT) * factor - norm)
        far = weights * (dot(gs, far_v, NT) - delta)
        parts = []
        for turn in range(top):
            part = far[:, turn * block_len:(turn + 1) * block_len]
            parts.append(jnp.where(sel_of(pair * top + turn) >= 0, part, 0.0))
        far = jnp.concatenate(parts, axis=1).astype(jnp.bfloat16)
        total = ((dot(near, own_k, NN) + dot(far, far_k, NN)) * factor).astype(dq_ref.dtype)
        step = min(size, block_len)
        for start in range(0, block_len, step):
            row = block * block_len + start
            chunk = (row // size + chunks - mine) % chunks
            dq_ref[chunk, row % size:row % size + step, head * dh:(head + 1) * dh] = total[start:start + step]


def owner_kernel(
    blocks, heads, block_len, dh, factor,
    q_ref, g_ref, k_ref, v_ref, own_ref, m_buf, a_buf, b_buf,
    dk_ref, dv_ref,
    jq, jg, kacc, vacc, tab_ref, job_src, job_pair, job_key, job_sem, tab_sem,
):
    me = lax.axis_index("ctx")
    count = m_buf.shape[0]
    pairs = blocks * heads
    place = (block_len, dh)

    fetch_table = pltpu.make_async_copy(m_buf.at[:, pl.ds(2 * pairs, PER_PEER), :], tab_ref, tab_sem)
    fetch_table.start()
    fetch_table.wait()

    def scan(dev, found):
        for rank in range(PER_PEER):
            code = tab_ref[dev, rank, me].astype(jnp.int32)
            pair = code // blocks
            block, head = pair // heads, pair % heads

            @pl.when(code >= 0)
            def _():
                job_src[found] = dev
                job_pair[found] = pair
                job_key[found] = (code % blocks) * heads + head
                row = pl.multiple_of(block * block_len, block_len)
                col = pl.multiple_of(head * dh, dh)
                spot = (dev, pl.ds(row, block_len), pl.ds(col, dh))
                pltpu.make_async_copy(a_buf.at[spot], jq.at[found], job_sem.at[0, found]).start()
                pltpu.make_async_copy(b_buf.at[spot], jg.at[found], job_sem.at[1, found]).start()

            found = found + (code >= 0).astype(jnp.int32)
        return found

    found = lax.fori_loop(me + 1, count, scan, jnp.int32(0))

    def owner_terms(keys, vals, qs, gs, norm, delta, causal):
        scores = dot(keys, qs, NT) * factor
        weights = jnp.exp(scores - norm)
        if causal:
            at_key = lax.broadcasted_iota(jnp.int32, scores.shape, 0)
            at_query = lax.broadcasted_iota(jnp.int32, scores.shape, 1)
            weights = jnp.where(at_key <= at_query, weights, 0.0)
        dweights = dot(vals, gs, NT)
        dscores = (weights * (dweights - delta)).astype(jnp.bfloat16)
        return dot(dscores, qs, NN) * factor, dot(weights.astype(jnp.bfloat16), gs, NN)

    for pair in range(pairs):
        block, head = pair // heads, pair % heads
        part_k, part_v = owner_terms(
            piece(k_ref, block, head, *place), piece(v_ref, block, head, *place),
            piece(q_ref, block, head, *place), piece(g_ref, block, head, *place),
            own_ref[pair:pair + 1, :], own_ref[pairs + pair:pairs + pair + 1, :], True,
        )
        kacc[pair] = part_k
        vacc[pair] = part_v

    def drain(job, carry):
        pltpu.make_async_copy(view(k_ref, 0, 0, *place), jq.at[job], job_sem.at[0, job]).wait()
        pltpu.make_async_copy(view(v_ref, 0, 0, *place), jg.at[job], job_sem.at[1, job]).wait()
        return carry

    lax.fori_loop(0, found, drain, 0)

    def turn(step, carry):
        results = []
        for lane in range(JOBS_STEP):
            job = step * JOBS_STEP + lane
            live = job < found
            job = jnp.minimum(job, found - 1)
            key = job_key[job]
            src, pair = job_src[job], job_pair[job]
            block, head = key // heads, key % heads
            rows = pl.ds(pl.multiple_of(block * block_len, block_len), block_len)
            cols = pl.ds(pl.multiple_of(head * dh, dh), dh)
            part_k, part_v = owner_terms(
                k_ref[rows, cols], v_ref[rows, cols], jq[job], jg[job],
                m_buf[src, pl.ds(pair, 1), :], m_buf[src, pl.ds(pairs + pair, 1), :], False,
            )
            results.append((key, jnp.where(live, part_k, 0.0), jnp.where(live, part_v, 0.0)))
        for key, part_k, part_v in results:
            kacc[key] += part_k
            vacc[key] += part_v
        return carry

    lax.fori_loop(0, (found + JOBS_STEP - 1) // JOBS_STEP, turn, 0)
    for pair in range(pairs):
        block, head = pair // heads, pair % heads
        rows = slice(block * block_len, (block + 1) * block_len)
        dk_ref[rows, head * dh:(head + 1) * dh] = kacc[pair].astype(dk_ref.dtype)
        dv_ref[rows, head * dh:(head + 1) * dh] = vacc[pair].astype(dv_ref.dtype)


def join_kernel(chunk_ref, *refs):
    moved, out_ref = refs[:-1], refs[-1]
    chunks, size, width = chunk_ref.shape
    mine = lax.axis_index("head")
    for shift in range(chunks):
        source = (mine + chunks - shift) % chunks
        cols = pl.ds(pl.multiple_of(source * width, width), width)
        out_ref[:, cols] = chunk_ref[0] if shift == 0 else moved[shift - 1][...]


def prep_kernel(blocks, heads, top, block_len, dh, sel_ref, g_ref, o_ref, n_ref, stat_ref, meta_ref):
    pairs = blocks * heads
    lanes = lax.broadcasted_iota(jnp.int32, (block_len, block_len), 1)
    for block in range(blocks):
        rows = slice(block * block_len, (block + 1) * block_len)
        table = jnp.zeros((block_len, block_len), jnp.float32)
        for head in range(heads):
            cols = slice(head * dh, (head + 1) * dh)
            terms = g_ref[rows, cols].astype(jnp.float32) * o_ref[rows, cols].astype(jnp.float32)
            delta = jnp.sum(terms, axis=1, keepdims=True)
            table = jnp.where(lanes == heads + head, delta, table)
        norms = n_ref[:, rows]
        spread = jnp.concatenate([norms, jnp.zeros((block_len - heads, block_len), jnp.float32)], axis=0)
        stat_ref[rows, :] = (table + jnp.transpose(spread))[:, :2 * heads]
        turned = jnp.transpose(table)
        meta_ref[block * heads:(block + 1) * heads, :] = norms
        meta_ref[pairs + block * heads:pairs + (block + 1) * heads, :] = turned[heads:2 * heads]
    lane = lax.broadcasted_iota(jnp.int32, (8, block_len), 1)
    slots = [jnp.full((8, block_len), -1, jnp.int32) for _ in range(PER_PEER)]
    for entry in range(pairs * top):
        value = sel_ref[entry % top, entry // top // heads, entry // top % heads]
        owner = jnp.where(value >= 0, value // blocks, -1)
        code = (entry // top) * blocks + value % blocks
        here = lane == owner
        for rank in range(PER_PEER):
            free = slots[rank] < 0
            slots[rank] = jnp.where(here & free, code, slots[rank])
            here = here & jnp.logical_not(free)
    row = lax.broadcasted_iota(jnp.int32, (8, block_len), 0)
    table = jnp.zeros((8, block_len), jnp.int32)
    for rank in range(PER_PEER):
        table = jnp.where(row == rank, slots[rank], table)
    meta_ref[2 * pairs:2 * pairs + 8, :] = table.astype(jnp.float32)


def shards(queries, keys, values, out_grad, outputs, log_norms, selected):
    blocks, heads, top = selected.shape
    row_count, width = queries.shape
    dh = width // heads
    block_len = row_count // blocks
    pairs = blocks * heads
    count = lax.axis_size("ctx")
    per_dev = pairs * top
    vmem = pl.BlockSpec(memory_space=pltpu.VMEM)
    smem = pl.BlockSpec(memory_space=pltpu.SMEM)
    anywhere = pl.BlockSpec(memory_space=pl.ANY)
    chosen = jnp.transpose(selected, (2, 0, 1))
    stats, meta = pl.pallas_call(
        functools.partial(prep_kernel, blocks, heads, top, block_len, dh),
        out_shape=(
            jax.ShapeDtypeStruct((row_count, 2 * heads), jnp.float32),
            jax.ShapeDtypeStruct((2 * pairs + 8, block_len), jnp.float32),
        ),
        in_specs=[smem] + [vmem] * 3,
        out_specs=(vmem,) * 2,
    )(chosen, out_grad, outputs, jnp.transpose(log_norms))
    a_buf, b_buf, m_buf = gather(queries, out_grad, keys, values, meta)
    job_max = PER_PEER * count
    chunks = lax.axis_size("head")
    factor = dh ** (-0.5)
    spare = pltpu.VMEM((per_dev, block_len, dh), jnp.bfloat16)
    chunk_q = pl.pallas_call(
        functools.partial(query_kernel, blocks, heads, top, block_len, dh, factor),
        out_shape=jax.ShapeDtypeStruct((chunks, row_count // chunks, width), jnp.bfloat16),
        in_specs=[smem] + [vmem] * 5 + [anywhere] * 2,
        out_specs=vmem,
        scratch_shapes=[spare, spare, pltpu.SemaphoreType.DMA((2, per_dev))],
        cost_estimate=pl.CostEstimate(flops=10**9, bytes_accessed=4 * 10**6, transcendentals=10**6),
    )(chosen, queries, out_grad, keys, values, stats, a_buf, b_buf)
    moved = []
    for shift in range(1, chunks):
        ring = [(at, (at + shift) % chunks) for at in range(chunks)]
        moved.append(lax.ppermute(chunk_q[shift], "head", ring))
    grads = jax.ShapeDtypeStruct(queries.shape, jnp.bfloat16)
    jobs = pltpu.VMEM((job_max, block_len, dh), jnp.bfloat16)
    sums = pltpu.VMEM((pairs, block_len, dh), jnp.float32)
    grad_k, grad_v = pl.pallas_call(
        functools.partial(owner_kernel, blocks, heads, block_len, dh, factor),
        out_shape=(grads,) * 2,
        in_specs=[vmem] * 6 + [anywhere] * 2,
        out_specs=(vmem,) * 2,
        scratch_shapes=[
            jobs, jobs, sums, sums,
            pltpu.SMEM((count, PER_PEER, block_len), jnp.float32),
            pltpu.SMEM((job_max,), jnp.int32),
            pltpu.SMEM((job_max,), jnp.int32),
            pltpu.SMEM((job_max,), jnp.int32),
            pltpu.SemaphoreType.DMA((2, job_max)),
            pltpu.SemaphoreType.DMA,
        ],
        cost_estimate=pl.CostEstimate(flops=4 * 10**9, bytes_accessed=8 * 10**6, transcendentals=10**6),
    )(queries, out_grad, keys, values, meta, m_buf, a_buf, b_buf)
    spread_q = pl.pallas_call(
        join_kernel,
        out_shape=jax.ShapeDtypeStruct((row_count // chunks, chunks * width), jnp.bfloat16),
        in_specs=[vmem] * chunks,
        out_specs=vmem,
    )(chunk_q, *moved)
    return (spread_q, grad_k, grad_v)


def solution(mesh):
    placed = (P("ctx", "head"),) * 6 + (P("ctx", "head", None),)
    return jax.shard_map(
        shards,
        mesh=mesh,
        in_specs=placed,
        out_specs=(P(("ctx", "head"), None), P("ctx", "head"), P("ctx", "head")),
        check_vma=False,
    )
```

```python
import functools

import jax
import jax.numpy as jnp
from jax import lax
from jax.experimental import pallas as pl
from jax.experimental.pallas import tpu as pltpu
from jax.sharding import PartitionSpec as P

GROUP = 4
JOBS_STEP = 6
PER_PEER = 2
MESH_ID = pl.DeviceIdType.MESH
NT = (((1,), (1,)), ((), ()))
NN = (((1,), (0,)), ((), ()))


def gather_kernel(levels, q_ref, g_ref, k_ref, v_ref, m_ref, a_buf, b_buf, m_buf, send_sem, recv_sem):
    me = lax.axis_index("ctx")
    head = lax.axis_index("head")
    level = me // GROUP
    col = me % GROUP
    colx = (col + 2) % GROUP
    colc = col + 1 - 2 * (col % 2)
    down_dev = me - GROUP
    up_dev = me + GROUP
    x_dev = level * GROUP + colx
    c_dev = level * GROUP + colc
    bufs = (a_buf, b_buf, m_buf)
    down_own = (q_ref, g_ref, m_ref)
    up_own = (k_ref, v_ref, m_ref)
    has_down = level > 0
    has_up = level < levels - 1

    barrier = pltpu.get_barrier_semaphore()

    def greet(dev):
        pl.semaphore_signal(barrier, inc=1, device_id=(dev, head), device_id_type=MESH_ID)

    greet(x_dev)
    greet(c_dev)

    @pl.when(has_down)
    def _():
        greet(down_dev)

    @pl.when(has_up)
    def _():
        greet(up_dev)

    pl.semaphore_wait(barrier, 2 + has_down.astype(jnp.int32) + has_up.astype(jnp.int32))

    def copy(way, part, slot, src, dev):
        return pltpu.make_async_remote_copy(
            src_ref=src,
            dst_ref=bufs[part].at[slot],
            send_sem=send_sem.at[way, part, slot],
            recv_sem=recv_sem.at[part, slot],
            device_id=(dev, head),
            device_id_type=MESH_ID,
        )

    def push(way, slot, dev, own=None):
        for part in (2, 0, 1):
            src = bufs[part].at[slot] if own is None else own[part]
            copy(way, part, slot, src, dev).start()

    def push_part(way, part, slot, dev):
        copy(way, part, slot, bufs[part].at[slot], dev).start()

    def arrive(part, slot):
        copy(0, part, slot, bufs[part].at[slot], c_dev).wait_recv()

    def sent(way, slot, which=(0, 1, 2)):
        for part in which:
            copy(way, part, slot, bufs[part].at[slot], c_dev).wait_send()

    @pl.when(has_down)
    def _():
        push(0, me, down_dev, down_own)

    @pl.when(has_up)
    def _():
        push(3, me, up_dev, up_own)

    @pl.when(col >= 2)
    def _():
        push(1, me, x_dev, down_own)

    @pl.when(col < 2)
    def _():
        push(1, me, x_dev, up_own)

    @pl.when(col % 2 == 1)
    def _():
        push(2, me, c_dev, down_own)

    @pl.when(col % 2 == 0)
    def _():
        push(2, me, c_dev, up_own)

    def by_edge(other):
        skip_low = (level == 0) & (other == 2)
        skip_high = (level == levels - 1) & (other == levels - 3)
        return skip_low | skip_high

    def relay_low(other):
        return (level == 1) & (other == 2)

    def relay_high(other):
        return (level == levels - 2) & (other == levels - 3)

    def cross(other):
        slot = other * GROUP + colx
        for part in (2, 0, 1):
            arrive(part, slot)
            if part == 0:

                @pl.when(relay_low(other))
                def _():
                    push_part(4, part, slot, down_dev)

                @pl.when(relay_high(other))
                def _():
                    push_part(4, part, slot, up_dev)

            push_part(2, part, slot, c_dev)

    def push_across(part, other, slot):
        if part == 0:

            @pl.when(jnp.logical_not(by_edge(other)))
            def _():
                push_part(1, part, slot, x_dev)

        else:
            push_part(1, part, slot, x_dev)

    def step(dist, carry):
        high = level + dist
        low = level - dist

        @pl.when(high < levels)
        def _():
            slot = high * GROUP + col
            for part in (2, 0, 1):
                arrive(part, slot)

                @pl.when(has_down)
                def _():
                    push_part(0, part, slot, down_dev)

                push_across(part, high, slot)
                push_part(2, part, slot, c_dev)

        @pl.when(low >= 0)
        def _():
            slot = low * GROUP + col
            for part in (2, 0, 1):
                arrive(part, slot)

                @pl.when(has_up)
                def _():
                    push_part(0, part, slot, up_dev)

                push_across(part, low, slot)
                push_part(2, part, slot, c_dev)

        before = dist - 1

        @pl.when(level + before < levels)
        def _():
            cross(level + before)

        @pl.when((before > 0) & (level - before >= 0))
        def _():
            cross(level - before)

        return carry

    lax.fori_loop(1, levels + 1, step, 0)

    def finish(other, carry):
        for column in (colc, (colc + 2) % GROUP):
            for part in range(3):
                arrive(part, other * GROUP + column)
        own_slot = other * GROUP + col
        sent(1, own_slot, (1, 2))

        @pl.when(jnp.logical_not(by_edge(other)))
        def _():
            sent(1, own_slot, (0,))

        @pl.when(relay_low(other) | relay_high(other))
        def _():
            sent(4, other * GROUP + colx, (0,))

        sent(2, own_slot)
        sent(2, other * GROUP + colx)

        @pl.when(has_down & (other >= level))
        def _():
            sent(0, own_slot)

        @pl.when(has_up & (other < level))
        def _():
            sent(0, own_slot)

        @pl.when(has_up & (other == level))
        def _():
            sent(3, own_slot)

        return carry

    lax.fori_loop(0, levels, finish, 0)


def gather(queries, out_grad, keys, values, meta):
    count = lax.axis_size("ctx")
    rows = queries.shape
    anywhere = pl.BlockSpec(memory_space=pl.ANY)
    return pl.pallas_call(
        functools.partial(gather_kernel, count // GROUP),
        out_shape=(
            jax.ShapeDtypeStruct((count,) + rows, queries.dtype),
            jax.ShapeDtypeStruct((count,) + rows, queries.dtype),
            jax.ShapeDtypeStruct((count,) + meta.shape, meta.dtype),
        ),
        in_specs=[anywhere] * 5,
        out_specs=(anywhere,) * 3,
        scratch_shapes=[
            pltpu.SemaphoreType.DMA((5, 3, count)),
            pltpu.SemaphoreType.DMA((3, count)),
        ],
        compiler_params=pltpu.CompilerParams(collective_id=0, has_side_effects=True),
    )(queries, out_grad, keys, values, meta)


def dot(left, right, dims):
    return lax.dot_general(left, right, dims, preferred_element_type=jnp.float32)


def piece(ref, block, head, block_len, dh):
    return ref[block * block_len:(block + 1) * block_len, head * dh:(head + 1) * dh]


def view(ref, block, head, block_len, dh):
    return ref.at[pl.ds(block * block_len, block_len), pl.ds(head * dh, dh)]


def far_view(ref, dev, block, head, block_len, dh):
    return ref.at[dev, pl.ds(block * block_len, block_len), pl.ds(head * dh, dh)]


def query_kernel(
    blocks, heads, top, block_len, dh, factor,
    sel_ref, q_ref, g_ref, k_ref, v_ref, stat_ref, a_buf, b_buf, dq_ref, sk, sv, sel_sem,
):
    chunks, size = dq_ref.shape[0], dq_ref.shape[1]
    mine = lax.axis_index("head")
    pairs = blocks * heads
    per_dev = pairs * top
    place = (block_len, dh)

    def sel_of(entry):
        return sel_ref[entry % top, entry // top // heads, entry // top % heads]

    for entry in range(per_dev):
        chosen = sel_of(entry)
        block, head = entry // top // heads, entry // top % heads

        @pl.when(chosen >= 0)
        def _():
            dev, inner = chosen // blocks, chosen % blocks
            pltpu.make_async_copy(far_view(a_buf, dev, inner, head, *place), sk.at[entry], sel_sem.at[0, entry]).start()
            pltpu.make_async_copy(far_view(b_buf, dev, inner, head, *place), sv.at[entry], sel_sem.at[1, entry]).start()

        @pl.when(chosen < 0)
        def _():
            pltpu.make_async_copy(view(k_ref, block, head, *place), sk.at[entry], sel_sem.at[0, entry]).start()
            pltpu.make_async_copy(view(v_ref, block, head, *place), sv.at[entry], sel_sem.at[1, entry]).start()

    for entry in range(per_dev):
        pltpu.make_async_copy(view(k_ref, 0, 0, *place), sk.at[entry], sel_sem.at[0, entry]).wait()
        pltpu.make_async_copy(view(v_ref, 0, 0, *place), sv.at[entry], sel_sem.at[1, entry]).wait()
    wide = top * block_len
    for pair in range(pairs):
        block, head = pair // heads, pair % heads
        qs, gs = piece(q_ref, block, head, *place), piece(g_ref, block, head, *place)
        own_k, own_v = piece(k_ref, block, head, *place), piece(v_ref, block, head, *place)
        rows = slice(block * block_len, (block + 1) * block_len)
        norm = stat_ref[rows, head:head + 1]
        delta = stat_ref[rows, heads + head:heads + head + 1]
        far_k = sk[pair * top:(pair + 1) * top].reshape(wide, dh)
        far_v = sv[pair * top:(pair + 1) * top].reshape(wide, dh)
        weights = jnp.exp(dot(qs, own_k, NT) * factor - norm)
        at_query = lax.broadcasted_iota(jnp.int32, weights.shape, 0)
        at_key = lax.broadcasted_iota(jnp.int32, weights.shape, 1)
        weights = jnp.where(at_key <= at_query, weights, 0.0)
        near = (weights * (dot(gs, own_v, NT) - delta)).astype(jnp.bfloat16)
        weights = jnp.exp(dot(qs, far_k, NT) * factor - norm)
        far = weights * (dot(gs, far_v, NT) - delta)
        parts = []
        for turn in range(top):
            part = far[:, turn * block_len:(turn + 1) * block_len]
            parts.append(jnp.where(sel_of(pair * top + turn) >= 0, part, 0.0))
        far = jnp.concatenate(parts, axis=1).astype(jnp.bfloat16)
        total = ((dot(near, own_k, NN) + dot(far, far_k, NN)) * factor).astype(dq_ref.dtype)
        step = min(size, block_len)
        for start in range(0, block_len, step):
            row = block * block_len + start
            chunk = (row // size + chunks - mine) % chunks
            dq_ref[chunk, row % size:row % size + step, head * dh:(head + 1) * dh] = total[start:start + step]


def owner_kernel(
    blocks, heads, block_len, dh, factor,
    q_ref, g_ref, k_ref, v_ref, own_ref, m_buf, a_buf, b_buf,
    dk_ref, dv_ref,
    jq, jg, kacc, vacc, tab_ref, job_src, job_pair, job_key, job_sem, tab_sem,
):
    me = lax.axis_index("ctx")
    count = m_buf.shape[0]
    pairs = blocks * heads
    place = (block_len, dh)

    fetch_table = pltpu.make_async_copy(m_buf.at[:, pl.ds(2 * pairs, PER_PEER), :], tab_ref, tab_sem)
    fetch_table.start()
    fetch_table.wait()

    def scan(dev, found):
        for rank in range(PER_PEER):
            code = tab_ref[dev, rank, me].astype(jnp.int32)
            pair = code // blocks
            block, head = pair // heads, pair % heads

            @pl.when(code >= 0)
            def _():
                job_src[found] = dev
                job_pair[found] = pair
                job_key[found] = (code % blocks) * heads + head
                row = pl.multiple_of(block * block_len, block_len)
                col = pl.multiple_of(head * dh, dh)
                spot = (dev, pl.ds(row, block_len), pl.ds(col, dh))
                pltpu.make_async_copy(a_buf.at[spot], jq.at[found], job_sem.at[0, found]).start()
                pltpu.make_async_copy(b_buf.at[spot], jg.at[found], job_sem.at[1, found]).start()

            found = found + (code >= 0).astype(jnp.int32)
        return found

    found = lax.fori_loop(me + 1, count, scan, jnp.int32(0))

    def owner_terms(keys, vals, qs, gs, norm, delta, causal):
        scores = dot(keys, qs, NT) * factor
        weights = jnp.exp(scores - norm)
        if causal:
            at_key = lax.broadcasted_iota(jnp.int32, scores.shape, 0)
            at_query = lax.broadcasted_iota(jnp.int32, scores.shape, 1)
            weights = jnp.where(at_key <= at_query, weights, 0.0)
        dweights = dot(vals, gs, NT)
        dscores = (weights * (dweights - delta)).astype(jnp.bfloat16)
        return dot(dscores, qs, NN) * factor, dot(weights.astype(jnp.bfloat16), gs, NN)

    for pair in range(pairs):
        block, head = pair // heads, pair % heads
        part_k, part_v = owner_terms(
            piece(k_ref, block, head, *place), piece(v_ref, block, head, *place),
            piece(q_ref, block, head, *place), piece(g_ref, block, head, *place),
            own_ref[pair:pair + 1, :], own_ref[pairs + pair:pairs + pair + 1, :], True,
        )
        kacc[pair] = part_k
        vacc[pair] = part_v

    def drain(job, carry):
        pltpu.make_async_copy(view(k_ref, 0, 0, *place), jq.at[job], job_sem.at[0, job]).wait()
        pltpu.make_async_copy(view(v_ref, 0, 0, *place), jg.at[job], job_sem.at[1, job]).wait()
        return carry

    lax.fori_loop(0, found, drain, 0)

    def turn(step, carry):
        results = []
        for lane in range(JOBS_STEP):
            job = step * JOBS_STEP + lane
            live = job < found
            job = jnp.minimum(job, found - 1)
            key = job_key[job]
            src, pair = job_src[job], job_pair[job]
            block, head = key // heads, key % heads
            rows = pl.ds(pl.multiple_of(block * block_len, block_len), block_len)
            cols = pl.ds(pl.multiple_of(head * dh, dh), dh)
            part_k, part_v = owner_terms(
                k_ref[rows, cols], v_ref[rows, cols], jq[job], jg[job],
                m_buf[src, pl.ds(pair, 1), :], m_buf[src, pl.ds(pairs + pair, 1), :], False,
            )
            results.append((key, jnp.where(live, part_k, 0.0), jnp.where(live, part_v, 0.0)))
        for key, part_k, part_v in results:
            kacc[key] += part_k
            vacc[key] += part_v
        return carry

    lax.fori_loop(0, (found + JOBS_STEP - 1) // JOBS_STEP, turn, 0)
    for pair in range(pairs):
        block, head = pair // heads, pair % heads
        rows = slice(block * block_len, (block + 1) * block_len)
        dk_ref[rows, head * dh:(head + 1) * dh] = kacc[pair].astype(dk_ref.dtype)
        dv_ref[rows, head * dh:(head + 1) * dh] = vacc[pair].astype(dv_ref.dtype)


def join_kernel(chunk_ref, *refs):
    moved, out_ref = refs[:-1], refs[-1]
    chunks, size, width = chunk_ref.shape
    mine = lax.axis_index("head")
    for shift in range(chunks):
        source = (mine + chunks - shift) % chunks
        cols = pl.ds(pl.multiple_of(source * width, width), width)
        out_ref[:, cols] = chunk_ref[0] if shift == 0 else moved[shift - 1][...]


def prep_kernel(blocks, heads, top, block_len, dh, sel_ref, g_ref, o_ref, n_ref, stat_ref, meta_ref):
    pairs = blocks * heads
    lanes = lax.broadcasted_iota(jnp.int32, (block_len, block_len), 1)
    for block in range(blocks):
        rows = slice(block * block_len, (block + 1) * block_len)
        table = jnp.zeros((block_len, block_len), jnp.float32)
        for head in range(heads):
            cols = slice(head * dh, (head + 1) * dh)
            terms = g_ref[rows, cols].astype(jnp.float32) * o_ref[rows, cols].astype(jnp.float32)
            delta = jnp.sum(terms, axis=1, keepdims=True)
            table = jnp.where(lanes == heads + head, delta, table)
        norms = n_ref[:, rows]
        spread = jnp.concatenate([norms, jnp.zeros((block_len - heads, block_len), jnp.float32)], axis=0)
        stat_ref[rows, :] = (table + jnp.transpose(spread))[:, :2 * heads]
        turned = jnp.transpose(table)
        meta_ref[block * heads:(block + 1) * heads, :] = norms
        meta_ref[pairs + block * heads:pairs + (block + 1) * heads, :] = turned[heads:2 * heads]
    lane = lax.broadcasted_iota(jnp.int32, (8, block_len), 1)
    slots = [jnp.full((8, block_len), -1, jnp.int32) for _ in range(PER_PEER)]
    for entry in range(pairs * top):
        value = sel_ref[entry % top, entry // top // heads, entry // top % heads]
        owner = jnp.where(value >= 0, value // blocks, -1)
        code = (entry // top) * blocks + value % blocks
        here = lane == owner
        for rank in range(PER_PEER):
            free = slots[rank] < 0
            slots[rank] = jnp.where(here & free, code, slots[rank])
            here = here & jnp.logical_not(free)
    row = lax.broadcasted_iota(jnp.int32, (8, block_len), 0)
    table = jnp.zeros((8, block_len), jnp.int32)
    for rank in range(PER_PEER):
        table = jnp.where(row == rank, slots[rank], table)
    meta_ref[2 * pairs:2 * pairs + 8, :] = table.astype(jnp.float32)


def shards(queries, keys, values, out_grad, outputs, log_norms, selected):
    blocks, heads, top = selected.shape
    row_count, width = queries.shape
    dh = width // heads
    block_len = row_count // blocks
    pairs = blocks * heads
    count = lax.axis_size("ctx")
    per_dev = pairs * top
    vmem = pl.BlockSpec(memory_space=pltpu.VMEM)
    smem = pl.BlockSpec(memory_space=pltpu.SMEM)
    anywhere = pl.BlockSpec(memory_space=pl.ANY)
    chosen = jnp.transpose(selected, (2, 0, 1))
    stats, meta = pl.pallas_call(
        functools.partial(prep_kernel, blocks, heads, top, block_len, dh),
        out_shape=(
            jax.ShapeDtypeStruct((row_count, 2 * heads), jnp.float32),
            jax.ShapeDtypeStruct((2 * pairs + 8, block_len), jnp.float32),
        ),
        in_specs=[smem] + [vmem] * 3,
        out_specs=(vmem,) * 2,
    )(chosen, out_grad, outputs, jnp.transpose(log_norms))
    a_buf, b_buf, m_buf = gather(queries, out_grad, keys, values, meta)
    job_max = PER_PEER * count
    chunks = lax.axis_size("head")
    factor = dh ** (-0.5)
    spare = pltpu.VMEM((per_dev, block_len, dh), jnp.bfloat16)
    chunk_q = pl.pallas_call(
        functools.partial(query_kernel, blocks, heads, top, block_len, dh, factor),
        out_shape=jax.ShapeDtypeStruct((chunks, row_count // chunks, width), jnp.bfloat16),
        in_specs=[smem] + [vmem] * 5 + [anywhere] * 2,
        out_specs=vmem,
        scratch_shapes=[spare, spare, pltpu.SemaphoreType.DMA((2, per_dev))],
        cost_estimate=pl.CostEstimate(flops=10**9, bytes_accessed=4 * 10**6, transcendentals=10**6),
    )(chosen, queries, out_grad, keys, values, stats, a_buf, b_buf)
    moved = []
    for shift in range(1, chunks):
        ring = [(at, (at + shift) % chunks) for at in range(chunks)]
        moved.append(lax.ppermute(chunk_q[shift], "head", ring))
    grads = jax.ShapeDtypeStruct(queries.shape, jnp.bfloat16)
    jobs = pltpu.VMEM((job_max, block_len, dh), jnp.bfloat16)
    sums = pltpu.VMEM((pairs, block_len, dh), jnp.float32)
    grad_k, grad_v = pl.pallas_call(
        functools.partial(owner_kernel, blocks, heads, block_len, dh, factor),
        out_shape=(grads,) * 2,
        in_specs=[vmem] * 6 + [anywhere] * 2,
        out_specs=(vmem,) * 2,
        scratch_shapes=[
            jobs, jobs, sums, sums,
            pltpu.SMEM((count, PER_PEER, block_len), jnp.float32),
            pltpu.SMEM((job_max,), jnp.int32),
            pltpu.SMEM((job_max,), jnp.int32),
            pltpu.SMEM((job_max,), jnp.int32),
            pltpu.SemaphoreType.DMA((2, job_max)),
            pltpu.SemaphoreType.DMA,
        ],
        cost_estimate=pl.CostEstimate(flops=4 * 10**9, bytes_accessed=8 * 10**6, transcendentals=10**6),
    )(queries, out_grad, keys, values, meta, m_buf, a_buf, b_buf)
    spread_q = pl.pallas_call(
        join_kernel,
        out_shape=jax.ShapeDtypeStruct((row_count // chunks, chunks * width), jnp.bfloat16),
        in_specs=[vmem] * chunks,
        out_specs=vmem,
    )(chunk_q, *moved)
    return (spread_q, grad_k, grad_v)


def solution(mesh):
    placed = (P("ctx", "head"),) * 6 + (P("ctx", "head", None),)
    return jax.shard_map(
        shards,
        mesh=mesh,
        in_specs=placed,
        out_specs=(P(("ctx", "head"), None), P("ctx", "head"), P("ctx", "head")),
        check_vma=False,
    )
```
